32 devices in a mesh: rep: 1, dp: 32 (over x, y, z, core).
Axes of the slice: x: 2, y: 2, z: 4, core: 2. Of those that a mesh axis runs over, the one named last changes fastest.
Arguments:
- x: bfloat16 [32, 2048, 896], P(('rep', 'dp'))
- dy: bfloat16 [32, 2048, 896], P(('rep', 'dp'))
- wq: bfloat16 [2, 896, 1024], P(None, 'dp')
- wk: bfloat16 [2, 896, 512], P(None, 'dp')
- wv: bfloat16 [2, 896, 512], P(None, 'dp')
- wo: bfloat16 [2, 1024, 896], P(None, 'dp')
- w_gate: bfloat16 [2, 896, 3584], P(None, 'dp')
- w_up: bfloat16 [2, 896, 3584], P(None, 'dp')
- w_down: bfloat16 [2, 3584, 896], P(None, 'dp')
- m_wq: float32 [2, 896, 1024], P(None, 'dp')
- m_wk: float32 [2, 896, 512], P(None, 'dp')
- m_wv: float32 [2, 896, 512], P(None, 'dp')
- m_wo: float32 [2, 1024, 896], P(None, 'dp')
- m_w_gate: float32 [2, 896, 3584], P(None, 'dp')
- m_w_up: float32 [2, 896, 3584], P(None, 'dp')
- m_w_down: float32 [2, 3584, 896], P(None, 'dp')
- v_wq: float32 [2, 896, 1024], P(None, 'dp')
- v_wk: float32 [2, 896, 512], P(None, 'dp')
- v_wv: float32 [2, 896, 512], P(None, 'dp')
- v_wo: float32 [2, 1024, 896], P(None, 'dp')
- v_w_gate: float32 [2, 896, 3584], P(None, 'dp')
- v_w_up: float32 [2, 896, 3584], P(None, 'dp')
- v_w_down: float32 [2, 3584, 896], P(None, 'dp')
Outputs:
- output 1: bfloat16 [2, 896, 1024], P('rep', 'dp')
- output 2: bfloat16 [2, 896, 512], P('rep', 'dp')
- output 3: bfloat16 [2, 896, 512], P('rep', 'dp')
- output 4: bfloat16 [2, 1024, 896], P('rep', 'dp')
- output 5: bfloat16 [2, 896, 3584], P('rep', 'dp')
- output 6: bfloat16 [2, 896, 3584], P('rep', 'dp')
- output 7: bfloat16 [2, 3584, 896], P('rep', 'dp')
- output 8: float32 [2, 896, 1024], P('rep', 'dp')
- output 9: float32 [2, 896, 512], P('rep', 'dp')
- output 10: float32 [2, 896, 512], P('rep', 'dp')
- output 11: float32 [2, 1024, 896], P('rep', 'dp')
- output 12: float32 [2, 896, 3584], P('rep', 'dp')
- output 13: float32 [2, 896, 3584], P('rep', 'dp')
- output 14: float32 [2, 3584, 896], P('rep', 'dp')
- output 15: float32 [2, 896, 1024], P('rep', 'dp')
- output 16: float32 [2, 896, 512], P('rep', 'dp')
- output 17: float32 [2, 896, 512], P('rep', 'dp')
- output 18: float32 [2, 1024, 896], P('rep', 'dp')
- output 19: float32 [2, 896, 3584], P('rep', 'dp')
- output 20: float32 [2, 896, 3584], P('rep', 'dp')
- output 21: float32 [2, 3584, 896], P('rep', 'dp')
All inputs are finite; a program needn't handle non-finite values.
Results may differ from the reference program's by a relative error of at most 0.0289.
Values are sent between devices in bfloat16 or wider.
A program may use at most 2 GiB of HBM per device.

```python
import jax
import jax.numpy as jnp
from jax import lax

SEQUENCES = 32
TOKENS = 2048
D = 896
HEADS = 4
KV_HEADS = 2
HEAD = 256
FF = 3584
LAYERS = 2
THETA = 10000
NAMES = ("wq", "wk", "wv", "wo", "w_gate", "w_up", "w_down")
SHAPES = {
    "wq": (LAYERS, D, HEADS * HEAD),
    "wk": (LAYERS, D, KV_HEADS * HEAD),
    "wv": (LAYERS, D, KV_HEADS * HEAD),
    "wo": (LAYERS, HEADS * HEAD, D),
    "w_gate": (LAYERS, D, FF),
    "w_up": (LAYERS, D, FF),
    "w_down": (LAYERS, FF, D),
}


def bump(key, n, height):
    away = (jnp.arange(n, dtype=jnp.int32) - jax.random.randint(key, (), 0, n, jnp.int32)) % n
    return jnp.where(away < n // 8, height, 1.0)


def together(key, own, strength):
    shared = jax.random.normal(key, own.shape[1:], jnp.float32)
    return (own + strength * shared) * lax.rsqrt(1 + strength * strength)


def setup_inputs(seed: int = 0, part: int = 0) -> dict:
    kx, kdy, ka, kb, kz, kf, kh, kl, *keys = jax.random.split(jax.random.key(seed), 8 + 3 * len(NAMES))
    kx, kdy, ka, kb = (jax.random.fold_in(k, part) for k in (kx, kdy, ka, kb))
    kw, km, kv = (keys[i::3] for i in range(3))
    shape = (SEQUENCES, TOKENS, D)
    much_x, much_dy = jax.random.uniform(kz, (2,), jnp.float32, 0.0, 1.0)
    loud = 2.0 ** jax.random.uniform(jax.random.fold_in(kz, 1), (), jnp.float32, -1.0, 2.0)
    layers = 2.0 ** jax.random.uniform(kl, (LAYERS, 1, 1), jnp.float32, -1.0, 1.0)
    times = {"wq": 1.0, "wk": 1.0, "wv": 2.0, "wo": layers, "w_gate": 1.0, "w_up": bump(kh, FF, 4.0), "w_down": layers}
    x = together(ka, jax.random.normal(kx, shape, jnp.float32), much_x) * bump(kf, D, 4.0)
    dy = together(kb, jax.random.normal(kdy, shape, jnp.float32), much_dy)
    drawn = {"x": x.astype(jnp.bfloat16), "dy": (loud * dy * (SEQUENCES * TOKENS) ** -0.5).astype(jnp.bfloat16)}
    for key, name in zip(kw, NAMES, strict=True):
        drawn[name] = (jax.random.normal(key, SHAPES[name], jnp.float32) * SHAPES[name][1] ** -0.5 * times[name]).astype(jnp.bfloat16)
    for key, name in zip(km, NAMES, strict=True):
        drawn[f"m_{name}"] = 0.1 * jax.random.normal(key, SHAPES[name], jnp.float32)
    for key, name in zip(kv, NAMES, strict=True):
        drawn[f"v_{name}"] = jax.random.uniform(key, SHAPES[name], jnp.float32, 0.02, 0.06)
    return drawn


def matmul(a, w):
    return jnp.dot(a, w, preferred_element_type=jnp.float32).astype(jnp.bfloat16)


def normed(h):
    wide = h.astype(jnp.float32)
    scale = lax.rsqrt(jnp.mean(wide**2, -1, keepdims=True) + 1e-6)
    return (wide * scale).astype(jnp.bfloat16)


def turned(t, theta):
    half = t.shape[-1] // 2
    angle = jnp.arange(t.shape[0], dtype=jnp.float32)[:, None] * theta ** (-jnp.arange(half, dtype=jnp.float32) / half)
    cos, sin = jnp.cos(angle)[:, None], jnp.sin(angle)[:, None]
    a, b = t[..., :half].astype(jnp.float32), t[..., half:].astype(jnp.float32)
    return jnp.concatenate([a * cos - b * sin, b * cos + a * sin], -1).astype(jnp.bfloat16)


def seen_by(q, k, v):
    tokens, kv = q.shape[0], k.shape[1]
    q = q.reshape(tokens, kv, -1, q.shape[-1])
    scores = jnp.einsum("tgsd,ugd->gstu", q.astype(jnp.float32), k.astype(jnp.float32)) * q.shape[-1] ** -0.5
    place = jnp.arange(tokens)
    weights = jax.nn.softmax(jnp.where(place[:, None] >= place, scores, -jnp.inf), -1).astype(jnp.bfloat16)
    return jnp.einsum("gstu,ugd->tgsd", weights.astype(jnp.float32), v.astype(jnp.float32)).astype(jnp.bfloat16).reshape(tokens, -1)


def layer(h, w):
    a = normed(h)
    q, k = (turned(matmul(a, w[name]).reshape(h.shape[0], -1, HEAD), THETA) for name in ("wq", "wk"))
    h = h + matmul(seen_by(q, k, matmul(a, w["wv"]).reshape(h.shape[0], -1, HEAD)), w["wo"])
    b = normed(h)
    gate = jnp.dot(b, w["w_gate"], preferred_element_type=jnp.float32)
    up = jnp.dot(b, w["w_up"], preferred_element_type=jnp.float32)
    return h + matmul((jax.nn.silu(gate) * up).astype(jnp.bfloat16), w["w_down"])


def adamw(w, m, v, g):
    m = 0.9 * m + 0.1 * g
    v = 0.95 * v + 0.05 * g * g
    step = m * lax.rsqrt(v + 1e-8) + 0.1 * w
    return (w - 0.02 * step).astype(jnp.bfloat16), m, v


def clipped(gradients, sum_of_squares, count):
    factor = jnp.minimum(1.0, 0.5 * lax.rsqrt(sum_of_squares / count + 1e-30))
    return [g * factor for g in gradients]


def stack(weights, h):
    return lax.scan(lambda h, w: (layer(h, w), None), h, weights)[0]


def reference(x, dy, wq, wk, wv, wo, w_gate, w_up, w_down, m_wq, m_wk, m_wv, m_wo, m_w_gate, m_w_up, m_w_down, v_wq, v_wk, v_wv, v_wo, v_w_gate, v_w_up, v_w_down):
    weights = dict(zip(NAMES, (wq, wk, wv, wo, w_gate, w_up, w_down), strict=True))

    def take(so_far, sequence):
        h, by_y = sequence
        _, back = jax.vjp(stack, weights, h)
        by_weights, by_h = back(by_y)
        return jax.tree.map(lambda total, term: total + term.astype(jnp.float32), so_far, by_weights), by_h

    none_yet = {name: jnp.zeros(w.shape, jnp.float32) for name, w in weights.items()}
    by_weights, by_x = lax.scan(take, none_yet, (x, dy))
    gradients = [by_weights[name].astype(jnp.bfloat16).astype(jnp.float32) for name in NAMES]
    gradients = clipped(gradients, sum(jnp.sum(g * g) for g in gradients), sum(g.size for g in gradients))
    first = (m_wq, m_wk, m_wv, m_wo, m_w_gate, m_w_up, m_w_down)
    second = (v_wq, v_wk, v_wv, v_wo, v_w_gate, v_w_up, v_w_down)
    new = [adamw(weights[name].astype(jnp.float32), m, v, g) for name, m, v, g in zip(NAMES, first, second, gradients, strict=True)]
    return tuple(one[which] for which in range(3) for one in new)
```

```python
import functools

import jax
import jax.numpy as jnp
from jax import lax
from jax.experimental import pallas as pl
from jax.experimental.pallas import tpu as pltpu
from jax.sharding import PartitionSpec as P

T, D, F, HD, TILE = 2048, 896, 3584, 256, 512
HALF = HD // 2
CHIPS, LINES = 16, 4
OWN = 28
PAIR = 2 * OWN
LIMIT = 67043328
f32, bf16 = jnp.float32, jnp.bfloat16
THETA = 10000
HBM = pl.BlockSpec(memory_space=pltpu.HBM)


def dot(a, b, ca=1, cb=0):
    return lax.dot_general(a, b, (((ca,), (cb,)), ((), ())), preferred_element_type=f32)


def dot_t(a, b):
    return dot(a, b, 1, 1)


def t_dot(a, b):
    return dot(a, b, 0, 0)


def rms(h):
    return lax.rsqrt(jnp.mean(h * h, -1, keepdims=True) + 1e-6)


def normed(h):
    h = h.astype(f32)
    return (h * rms(h)).astype(bf16)


def norm_back(h, db, dres):
    s = rms(h)
    m = jnp.mean(h * db, -1, keepdims=True)
    return dres + (s * db - h * (s * s * s * m)).astype(bf16)


def const(*shape):
    return pl.BlockSpec(shape, lambda *i: (0,) * len(shape), pipeline_mode=pl.Buffered(1))


def shape(*dims, dtype=bf16):
    return jax.ShapeDtypeStruct(dims, dtype)


def block(at, n):
    return pl.ds(pl.multiple_of(at * n, n), n)


def place():
    me = lax.axis_index("dp")
    c, z, own = lax.rem(me, 2), lax.rem(lax.div(me, 2), LINES), lax.div(me, 2 * LINES)
    at = lambda line, z, c: (line * LINES + z) * 2 + c
    flip_x, flip_y = lax.rem(own + 2, LINES), own + 1 - 2 * lax.rem(own, 2)
    la, lb = jnp.where(c == 0, flip_y, flip_x), jnp.where(c == 0, flip_x, flip_y)
    peer = dict(d=at(own, z, 1 - c), a=at(la, z, c), b=at(lb, z, c))
    for k in range(1, LINES):
        peer[k] = at(own, lax.rem(z + k, LINES), c)
    return dict(c=c, z=z, own=own, la=la, lb=lb, ld=LINES - 1 - own, peer=peer)


def greet(pos):
    bar = pltpu.get_barrier_semaphore()
    for n in pos["peer"].values():
        pl.semaphore_signal(bar, inc=1, device_id=(0, n), device_id_type=pl.DeviceIdType.MESH)
    pl.semaphore_wait(bar, len(pos["peer"]))


def remote(src, dst, sems, i, device):
    return pltpu.make_async_remote_copy(src_ref=src, dst_ref=dst, send_sem=sems.at[0, i], recv_sem=sems.at[1, i], device_id=(0, device),
                                        device_id_type=pl.DeviceIdType.MESH)


class Gather:
    def __init__(self, pos, ref, cols, sems):
        self.pos, self.ref, self.cols, self.sems = pos, ref, cols, sems

    def part(self, chip, n):
        c = self.pos["c"]
        if len(self.ref.shape) > 3:
            return self.ref.at[pl.ds(chip, n), c]
        rows = block(chip if n == 1 else lax.div(chip, n), n * PAIR)
        return self.ref.at[c, rows] if self.cols is None else self.ref.at[c, rows, pl.ds(*self.cols)]

    def copies(self, what):
        p = self.pos
        peer, line = p["peer"], lambda name: self.part(LINES * p[name], LINES)
        mine = self.part(LINES * p["own"] + p["z"], 1)
        todo = dict(z=[(mine, k) for k in range(1, LINES)], ab=[(line("own"), "a"), (line("own"), "b")], far=[(line("la"), "b")],
                    near=[(line("own"), "d")], mid=[(line("la"), "d"), (line("lb"), "d")], last=[(line("ld"), "d")])
        first = 0
        for name, items in todo.items():
            if name == what:
                return [remote(src, src, self.sems, first + i, peer[to]) for i, (src, to) in enumerate(items)]
            first += len(items)

    def start(self, *names):
        for name in names:
            for copy in self.copies(name):
                copy.start()

    def wait(self, *names):
        for name in names:
            for copy in self.copies(name):
                copy.wait()


GATHER_SEMS = 10


class Ride:
    def __init__(self, refs, plan, sems, step, last):
        self.pos, self.plan, self.step, self.end = place(), plan, step, last
        self.parts = [Gather(self.pos, refs[name], cols, sems.at[i]) for i, (name, cols, *_) in enumerate(plan)]

    def at(self, k, todo):
        pl.when(self.step == k)(todo)

    def before(self):
        self.at(0, lambda: greet(self.pos))
        for part, (_, _, z, ab, far, end) in zip(self.parts, self.plan):
            if z is not None:
                self.at(z, lambda: part.start("z"))
            if ab is None:
                continue

            @functools.partial(self.at, ab)
            def _():
                if z is not None:
                    part.wait("z")
                part.start("ab", "near")

            @functools.partial(self.at, far)
            def _():
                part.wait("ab")
                part.start("far", "mid")

            if end < self.end:
                self.at(end, lambda: self.close(part))

    def close(self, part):
        part.wait("far")
        part.start("last")
        part.wait("near", "mid", "last")

    def after(self):
        @functools.partial(self.at, self.end)
        def _():
            late = [part for part, (*_, ab, _, end) in zip(self.parts, self.plan) if ab is not None and end >= self.end]
            for part in late:
                part.wait("far")
                part.start("last")
            for part, (_, _, z, ab, _, _) in zip(self.parts, self.plan):
                if z is not None and ab is None:
                    part.wait("z")
            for part in late:
                part.wait("near", "mid", "last")


def call(body, grid, ins, in_specs, out_specs, outs, scratch, flops, arrays=None, plan=(), cid=None):
    names = sorted({item[0] for item in plan})
    n_in, n_out, n_scratch, n = len(ins), len(outs), len(scratch), len(names)

    def kernel(*refs):
        given, refs = refs[:n_in], refs[n_in + n :]
        made, carried, refs = refs[:n_out], refs[n_out : n_out + n], refs[n_out + n :]
        step = pl.program_id(0)
        last = grid[0] - 1
        for i, size in enumerate(grid[1:]):
            step, last = step * size + pl.program_id(i + 1), (last + 1) * size - 1
        if not plan:
            return body(*given, *made, *refs)
        ride = Ride(dict(zip(names, carried)), plan, refs[n_scratch], step, last)
        ride.before()
        body(*given, *made, *refs[:n_scratch])
        ride.after()

    extra = [arrays[name] for name in names]
    got = pl.pallas_call(
        kernel, grid=grid, in_specs=list(in_specs) + [HBM] * n, out_specs=list(out_specs) + [HBM] * n,
        out_shape=list(outs) + [shape(*a.shape) for a in extra],
        scratch_shapes=list(scratch) + ([pltpu.SemaphoreType.DMA((len(plan), 2, GATHER_SEMS))] if plan else []),
        input_output_aliases={n_in + i: n_out + i for i in range(n)},
        compiler_params=pltpu.CompilerParams(vmem_limit_bytes=LIMIT, collective_id=cid, has_side_effects=bool(plan)),
        cost_estimate=pl.CostEstimate(flops=flops, bytes_accessed=flops // 1000, transcendentals=0),
    )(*ins, *extra)
    for name, new in zip(names, got[n_out:]):
        arrays[name] = new
    return got[:n_out]


def prologue_body(pack_ref, wo_ref, wd_ref, coarse_ref, fine_ref, cos_ref, sin_ref, qkv0, qkv1, gu0, gu1, wo0, wo1, wd0, wd1, theirs, merged, xs, ls, sems):
    pos = place()
    c, me = pos["c"], LINES * pos["own"] + pos["z"]
    greet(pos)
    across = [remote(pack_ref.at[1 - c, n], theirs.at[n], xs, n, pos["peer"]["d"]) for n in range(2)]
    for copy in across:
        copy.start()
    local = [pltpu.make_async_copy(w.at[n], ref.at[me, c], ls.at[i, n]) for i, (w, refs) in enumerate(((wo_ref, (wo0, wo1)), (wd_ref, (wd0, wd1)))) for n, ref in enumerate(refs)]
    for copy in local:
        copy.start()

    def merge(n, first, last):
        for at in range(first, last, TILE):
            cols = slice(at, at + TILE)
            mine, other = pack_ref[c, n, :, cols].astype(f32), theirs[n, :, cols].astype(f32)
            top, low = jnp.where(c == 0, mine, other), jnp.where(c == 0, other, mine)
            both = jnp.concatenate([top, low], 0)
            moved = pltpu.roll(both, both.shape[0] - (top.shape[0] - OWN), 0)
            row = lax.broadcasted_iota(jnp.int32, both.shape, 0)
            merged[n, :, cols] = jnp.where(row < OWN, both, moved)[:PAIR].astype(bf16)

    width = 2 * TILE

    def put(ref, n, first, size, i):
        copy = pltpu.make_async_copy(merged.at[n, :, pl.ds(first, size)], ref.at[c, block(me, PAIR)], ls.at[2 + i, n])
        copy.start()
        return copy

    halves = [Gather(pos, qkv0, (i * TILE, TILE), sems.at[i]) for i in range(2)]
    later = [Gather(pos, gu0, (0, F // 2), sems.at[2])]
    across[0].wait()
    merge(0, 0, width)
    put(qkv0, 0, 0, width, 0).wait()
    for part in halves:
        part.start("z")
    merge(0, width, width + F)
    there = put(gu0, 0, width, F, 1)
    across[1].wait()
    merge(1, 0, width + F)
    rest = [there, put(qkv1, 1, 0, width, 0), put(gu1, 1, width, F, 1)]
    there.wait()
    for part in later:
        part.start("z")
    for part in halves:
        part.wait("z")
        part.start("ab", "near")
    fine, big = fine_ref[:], coarse_ref[:]
    n = fine.shape[1]
    for i in range(T // n):
        rows = slice(i * n, i * n + n)
        ca, sa = big[0, i : i + 1], big[1, i : i + 1]
        cos_ref[rows, :] = ca * fine[0] - sa * fine[1]
        sin_ref[rows, :] = sa * fine[0] + ca * fine[1]
    for part in halves:
        part.wait("ab")
        part.start("far", "mid")
    for part in halves:
        part.wait("far")
        part.start("last")
    for copy in local + rest[1:]:
        copy.wait()
    for part in halves:
        part.wait("near", "mid", "last")
    for part in later:
        part.wait("z")


def prologue(pack, wo, wd, coarse, fine):
    rows = pack.shape[2]
    full = [shape(2, D, 2 * TILE)] * 2 + [shape(2, D, F)] * 2 + [shape(CHIPS, 2, wo.shape[1], D)] * 2 + [shape(CHIPS, 2, wd.shape[1], D)] * 2
    table = [shape(T, HALF, dtype=f32)] * 2
    whole = lambda a: const(*a.shape)
    got = pl.pallas_call(
        prologue_body, grid=(1,), in_specs=[whole(a) for a in (pack, wo, wd, coarse, fine)],
        out_specs=[whole(a) for a in table] + [HBM] * len(full), out_shape=table + full,
        scratch_shapes=[pltpu.VMEM((2, rows, pack.shape[3]), bf16), pltpu.VMEM((2, PAIR, pack.shape[3]), bf16), pltpu.SemaphoreType.DMA((2, 2)),
                        pltpu.SemaphoreType.DMA((LINES, 2)), pltpu.SemaphoreType.DMA((3, 2, GATHER_SEMS))],
        compiler_params=pltpu.CompilerParams(vmem_limit_bytes=LIMIT, collective_id=0, has_side_effects=True),
    )(pack, wo, wd, coarse, fine)
    return got[0], got[1], dict(zip(("qkv0", "qkv1", "gu0", "gu1", "wo0", "wo1", "wd0", "wd1"), got[2:]))


def turn(t, cos, sin):
    x, y = t[:, :HALF].astype(f32), t[:, HALF:].astype(f32)
    return jnp.concatenate([x * cos - y * sin, y * cos + x * sin], -1).astype(bf16)


def project_body(h_ref, w_ref, cos_ref, sin_ref, q_ref, k_ref, v_ref):
    a = normed(h_ref[:])
    cos, sin = cos_ref[:], sin_ref[:]
    for n, (owner, at, ref, head) in enumerate(((0, 0, q_ref, 0), (0, TILE, q_ref, 2), (1, 0, k_ref, 0), (1, TILE, v_ref, 0))):
        r = dot(a, w_ref[owner, :, at : at + TILE]).astype(bf16)
        for i in range(2):
            t = r[:, i * HD : i * HD + HD]
            ref[head + i] = turn(t, cos, sin) if ref is not v_ref else t


def project(h, w, cos, sin, *ride):
    rows = lambda width: pl.BlockSpec((TILE, width), lambda i: (i, 0))
    heads = (4, 2, 2)
    return call(project_body, (T // TILE,), (h, w, cos, sin), [rows(D), const(*w.shape), rows(HALF), rows(HALF)],
                [pl.BlockSpec((n, TILE, HD), lambda i: (0, i, 0)) for n in heads], [shape(n, T, HD) for n in heads], [], T * D * T * 2, *ride)


HIDDEN = -2e30
SCALE = HD**-0.5
EXP = SCALE * 1.4426950408889634
PIECES = [(i, n) for i in range(2) for n in range(2)]


def attend_body(q_ref, k_ref, v_ref, o_ref, lse_ref, top_s, mix_s):
    iq = pl.program_id(0)
    top_s[:] = jnp.full(top_s.shape, HIDDEN / 2, f32)
    mix_s[:] = jnp.zeros(mix_s.shape, f32)
    ones = jnp.ones((8, TILE), bf16)

    def keys(j, masked):
        here = block(j, TILE)
        scores = [dot_t(k_ref[i, here, :], q_ref[2 * i + n]) for i, n in PIECES]
        weights, keeps = [], []
        for m, s in enumerate(scores):
            if masked:
                s = jnp.where(lax.broadcasted_iota(jnp.int32, s.shape, 1) >= lax.broadcasted_iota(jnp.int32, s.shape, 0), s, HIDDEN)
            old = top_s[m : m + 1, :]
            top = jnp.maximum(old, s.max(axis=0, keepdims=True))
            top_s[m : m + 1, :] = top
            weights.append(jnp.exp2((s - top) * EXP).astype(bf16))
            keeps.append(jnp.exp2((old - top) * EXP))
        for m, (i, _) in enumerate(PIECES):
            values = jnp.concatenate([v_ref[i, here, :].T, ones], axis=0)
            mix_s[m] = mix_s[m] * keeps[m] + dot(values, weights[m])

    lax.fori_loop(0, iq, lambda j, _: keys(j, False), None)
    keys(iq, True)
    for m in range(len(PIECES)):
        total = mix_s[m, HD : HD + 1, :]
        o_ref[m] = (mix_s[m, :HD, :] * (1 / total)).T.astype(bf16)
        lse_ref[m] = top_s[m : m + 1, :] * SCALE + jnp.log(total)


def attend(q, k, v, *ride):
    tile = pl.BlockSpec((4, TILE, HD), lambda i: (0, i, 0))
    return call(attend_body, (T // TILE,), (q, k, v), [tile, const(*k.shape), const(*v.shape)],
                [tile, pl.BlockSpec((4, 1, TILE), lambda i: (0, 0, i))], [shape(4, T, HD), shape(4, 1, T, dtype=f32)],
                [pltpu.VMEM((4, TILE), f32), pltpu.VMEM((4, HD + 8, TILE), f32)], 4 * 2 * T * T * HD, *ride)


def gate_up_body(o_ref, wo_ref, h_ref, wg_ref, wu_ref, h2_ref, g_ref, u_ref, p_ref, b_s):
    j, t = pl.program_id(0), pl.program_id(1)
    tm = g_ref.shape[0]

    @pl.when(j == 0)
    def _():
        rows = block(t, tm)
        acc = sum(dot(o_ref[n, rows, :], wo_ref[4 * n : 4 * n + 4].reshape(HD, D)) for n in range(4))
        h2 = h_ref[rows, :] + acc.astype(bf16)
        h2_ref[rows, :] = h2
        b_s[rows, :] = normed(h2)

    sub = 256
    for m in range(tm // sub):
        here = slice(m * sub, m * sub + sub)
        b = b_s[block(t * (tm // sub) + m, sub), :]
        g, u = dot(b, wg_ref[0]), dot(b, wu_ref[0])
        g_ref[here, :] = g
        u_ref[here, :] = u
        p_ref[here, :] = (g * jax.nn.sigmoid(g) * u).astype(bf16)


def gate_up(o, wo, h, gu, *ride):
    tm = 1024
    tile = pl.BlockSpec((tm, TILE), lambda j, t: (t, j))
    weight = lambda i: pl.BlockSpec((1, D, TILE), lambda j, t: (i, 0, j))
    return call(gate_up_body, (F // TILE, T // tm), (o, wo, h, gu, gu), [const(*o.shape), const(*wo.shape), const(*h.shape), weight(0), weight(1)],
                [const(T, D), tile, tile, tile], [shape(T, D), shape(T, F, dtype=f32), shape(T, F, dtype=f32), shape(T, F)],
                [pltpu.VMEM((T, D), bf16)], 2 * T * D * (D + 2 * F), *ride)


def down_body(p_ref, wd_ref, h2_ref, h3_ref):
    acc = dot(p_ref[:], wd_ref[:])
    h3_ref[:] = h2_ref[:] + acc.astype(bf16)


def down(p, wd, h2, *ride):
    rows = lambda n: pl.BlockSpec((TILE, n), lambda i: (i, 0))
    return call(down_body, (T // TILE,), (p, wd.reshape(F, D), h2), [rows(F), const(F, D), rows(D)], [rows(D)], [shape(T, D)], [], 2 * T * D * F, *ride)


PLANS = (
    dict(project="gu0[0:4],-,0,2,9 gu0[4:8],0,-,-,- wo0,0,-,-,-",
         attend="wo0,-,0,1,9 gu0[4:8],-,0,2,9 wd0,0,-,-,-",
         gate_up="wd0,-,0,5,8 qkv1,0,8,11,99 wo1,0,8,11,99 gu1[0:2],8,-,-,-",
         down="gu1[0:2],-,0,2,9 gu1[2:4],0,-,-,-"),
    dict(project="gu1[2:4],-,0,2,9 gu1[4:8],0,-,-,-", attend="gu1[4:8],-,0,3,9 wd1,0,-,-,-", gate_up="wd1,-,0,6,12"),
)


def read_plan(text):
    name, *steps = text.split(",")
    name, _, cols = name.rstrip("]").partition("[")
    if cols:
        first, end = (F // 8 * int(n) for n in cols.split(":"))
        cols = (first, end - first)
    return name, cols or None, *(None if n == "-" else int(n) for n in steps)


def forward(x, pack, wo, wd, coarse, fine):
    cos, sin, arrays = prologue(pack, wo, wd, coarse, fine)
    h, kept, cid = x, [], 1
    for n, texts in enumerate(PLANS):
        plan = {name: [read_plan(item) for item in text.split()] for name, text in texts.items()}
        q, k, v = project(h, arrays[f"qkv{n}"], cos, sin, arrays, plan["project"], cid)
        o, lse = attend(q, k, v, arrays, plan["attend"], cid + 1)
        h2, g, u, p = gate_up(o, arrays[f"wo{n}"], h, arrays[f"gu{n}"], arrays, plan["gate_up"], cid + 2)
        kept.append((h, q, k, v, o, lse, h2, g, u, p))
        if n == 0:
            h, = down(p, arrays["wd0"], h2, arrays, plan["down"], cid + 3)
        cid += 4
    return cos, sin, arrays, kept


def ring_scratch(rows, width, slots=2):
    line = LINES * rows
    dims = ((2, LINES * line), (LINES * line,), (2, line), (line,), (LINES, rows), (LINES - 1, rows))
    return [pltpu.VMEM((slots, *d, width), bf16) for d in dims] + [pltpu.SemaphoreType.DMA((slots, 2, 7))]


RING = 7


class Ring:
    def __init__(self, pos, refs):
        self.pos = pos
        self.my, self.rd, self.rb, self.ra, self.zs, self.rz, self.sems = refs
        self.rows = self.zs.shape[2]

    def line(self, l):
        return block(l, LINES * self.rows)

    def copies(self, slot, stage):
        p, peer, sems = self.pos, self.pos["peer"], self.sems.at[slot]
        mine = self.my.at[slot, p["c"]]
        if stage == 0:
            return [remote(self.my.at[slot, 1 - p["c"]], self.rd.at[slot], sems, 0, peer["d"])]
        if stage == 1:
            return [remote(mine.at[self.line(p[name])], self.rb.at[slot, i], sems, 1 + i, peer["b"]) for i, name in enumerate(("lb", "ld"))]
        if stage == 2:
            return [remote(mine.at[self.line(p["la"])], self.ra.at[slot], sems, 3, peer["a"])]
        return [remote(self.zs.at[slot, lax.rem(p["z"] + k, LINES)], self.rz.at[slot, k - 1], sems, 3 + k, peer[k]) for k in range(1, LINES)]

    def send(self, slot, stage=0):
        for copy in self.copies(slot, stage):
            copy.start()

    def both(self, slot, l, theirs):
        return self.my[slot, self.pos["c"], self.line(l), :].astype(f32) + theirs.astype(f32)

    def add(self, slot, l, theirs):
        self.my[slot, self.pos["c"], self.line(l), :] = self.both(slot, l, theirs).astype(bf16)

    def stage(self, slot, n):
        p = self.pos
        for copy in self.copies(slot, n - 1):
            copy.wait()
        if n == 1:
            for l in range(LINES):
                self.add(slot, l, self.rd[slot, self.line(l), :])
        elif n == 2:
            self.add(slot, p["own"], self.rb[slot, 0])
            self.add(slot, p["la"], self.rb[slot, 1])
        elif n == 3:
            self.zs[slot] = self.both(slot, p["own"], self.ra[slot]).reshape(LINES, self.rows, -1).astype(bf16)
        else:
            return (self.zs[slot, p["z"]].astype(f32) + sum(self.rz[slot, k].astype(f32) for k in range(LINES - 1))).astype(bf16)
        self.send(slot, n)


def drain(units):
    while units:
        for ring, slot, n, end in units:
            ring.stage(slot, n) if n < 4 else end()
        units = [(ring, slot, n + 1, end) for ring, slot, n, end in units if n < 4]


def hand_over(pos, fin, out_ref, sems, local):
    c = pos["c"]
    across, here = remote(fin, out_ref.at[c], sems, 0, pos["peer"]["d"]), pltpu.make_async_copy(fin, out_ref.at[c], local)
    across.start()
    here.start()
    here.wait()
    across.wait()


def hand_scratch(width):
    return [pltpu.VMEM((PAIR, width), bf16), pltpu.SemaphoreType.DMA((2, 1)), pltpu.SemaphoreType.DMA(())]


def ffn_back_body(h2_ref, dy_ref, p_ref, g_ref, u_ref, wg_ref, wu_ref, wd_ref, gu_out, wd_out, dh_ref, b_s, db_s, dg_s, du_s, fin, xs, ls, *rest):
    j, t = pl.program_id(0), pl.program_id(1)
    tm, nj, nt = g_ref.shape[0], pl.num_programs(0), pl.num_programs(1) - 1
    pos = place()
    gu, wd = Ring(pos, rest[:RING]), Ring(pos, rest[RING:])
    slot, old = lax.rem(j, 2), lax.rem(j + 1, 2)
    third = lambda n: lax.rem(n, 3)
    pl.when((j == 0) & (t == 0))(lambda: greet(pos))

    def gu_end(slot, j):
        fin[:, block(j, TILE)] = gu.stage(slot, 4)

    def wd_end(slot, j):
        wd_out[:, block(j, HALF)] = wd.stage(slot, 4)

    has1, has2 = j >= 1, j >= 2

    @pl.when((t == 0) & has2)
    def _():
        gu.stage(slot, 3)
        wd.stage(third(j + 1), 2)

    pl.when((t == 1) & has1)(lambda: gu.stage(old, 1))

    @pl.when(t == 2)
    def _():
        pl.when(has1)(lambda: wd.stage(third(j + 2), 1))
        pl.when(has2)(lambda: wd.stage(third(j + 1), 3))

    pl.when((t == 3) & has2)(lambda: gu_end(slot, j - 2))

    @pl.when(t == 4)
    def _():
        pl.when(has1)(lambda: gu.stage(old, 2))
        pl.when(has2)(lambda: wd_end(third(j + 1), j - 2))

    sub = 256

    @pl.when(t < nt)
    def _():
        rows = block(t, tm)

        @pl.when(j == 0)
        def _():
            b_s[rows, :] = normed(h2_ref[rows, :])
            db_s[rows, :] = jnp.zeros((tm, D), f32)

        for m in range(tm // sub):
            here, rows = slice(m * sub, m * sub + sub), block(t * (tm // sub) + m, sub)
            dp = dot_t(dy_ref[rows, :], wd_ref[:]).astype(bf16).astype(f32)
            g, u = g_ref[here, :], u_ref[here, :]
            s = jax.nn.sigmoid(g)
            gs = g * s
            du = (dp * gs).astype(bf16)
            dg = (dp * u * (s + gs * (1 - s))).astype(bf16)
            dg_s[rows, :] = dg
            du_s[rows, :] = du
            db_s[rows, :] += dot_t(dg, wg_ref[0]) + dot_t(du, wu_ref[0])

        @pl.when(j == nj - 1)
        def _():
            for m in range(tm // sub):
                rows = block(t * (tm // sub) + m, sub)
                dh_ref[m * sub : m * sub + sub, :] = norm_back(h2_ref[rows, :].astype(f32), db_s[rows, :], dy_ref[rows, :])

    @pl.when(t == nt)
    def _():
        for i, ref in enumerate((dg_s, du_s)):
            for n in range(TILE // sub):
                cols = slice(sub * n, sub * n + sub)
                gu.my[slot, i, :, cols] = t_dot(b_s[:], ref[:, cols]).astype(bf16)
        gu.send(slot)
        rows = wd.rows
        for n in range(4):
            width = min(sub, D - sub * n)

            @pl.when(j == 2 * n)
            def _():
                for m in range(4):
                    r = t_dot(p_ref[:, D * m : D * m + D], dy_ref[:, sub * n : sub * n + width]).astype(bf16)
                    for q in range(8):
                        at = LINES * rows * m + rows * (q // 2)
                        for e in range(width // HALF):
                            wd.my[(2 * n + e) % 3, q % 2, at : at + rows, :] = r[rows * q : rows * q + rows, HALF * e : HALF * e + HALF]

        wd.send(third(j))

    @pl.when((t == nt) & (j == nj - 1))
    def _():
        last = F // TILE - 1
        old, slot, wd_old, wd_new = (last - 1) % 2, last % 2, (last - 1) % 3, last % 3
        drain([(gu, old, 3, lambda: gu_end(old, last - 1)), (wd, wd_old, 2, lambda: wd_end(wd_old, last - 1)),
               (gu, slot, 1, lambda: gu_end(slot, last)), (wd, wd_new, 1, lambda: wd_end(wd_new, last))])
        hand_over(pos, fin, gu_out, xs, ls)


def ffn_back(h2, dy, p, g, u, gu, wd, cid):
    tm = 512
    nj, nt = F // TILE, T // tm
    weight = lambda i: pl.BlockSpec((1, D, TILE), lambda j, t: (i, 0, j))
    tile = pl.BlockSpec((tm, TILE), lambda j, t: (jnp.minimum(t, nt - 1), j))
    rows = F // CHIPS // 2
    return pl.pallas_call(
        ffn_back_body, grid=(nj, nt + 1),
        in_specs=[const(T, D), const(T, D), const(T, F), tile, tile, weight(0), weight(1), pl.BlockSpec((TILE, D), lambda j, t: (j, 0))],
        out_specs=[HBM, const(rows, D), pl.BlockSpec((tm, D), lambda j, t: (jnp.where(j == nj - 1, jnp.minimum(t, nt - 1), 0), 0))],
        out_shape=[shape(2, PAIR, F), shape(rows, D), shape(T, D)],
        scratch_shapes=[pltpu.VMEM((T, D), bf16), pltpu.VMEM((T, D), f32), pltpu.VMEM((T, TILE), bf16), pltpu.VMEM((T, TILE), bf16)]
        + hand_scratch(F) + ring_scratch(PAIR, TILE) + ring_scratch(rows, HALF, 3),
        compiler_params=pltpu.CompilerParams(vmem_limit_bytes=LIMIT, collective_id=cid, has_side_effects=True),
        cost_estimate=pl.CostEstimate(flops=12 * T * D * F, bytes_accessed=F * T * 12, transcendentals=0),
    )(h2, dy, p, g, u, gu, gu, wd.reshape(F, D))


def out_back_body(o_ref, dh_ref, wo_ref, do_ref, delta_ref, dwo_ref):
    do = dot_t(dh_ref[:], wo_ref[:].reshape(HD, D)).astype(bf16)
    do_ref[0] = do
    o = o_ref[0]
    x = do.astype(f32) * o.astype(f32)
    delta_ref[0] = lax.dot_general(jnp.ones((8, HD), f32), x, (((1,), (1,)), ((), ())), precision=lax.Precision.HIGHEST, preferred_element_type=f32)[:1]
    r = t_dot(o, dh_ref[:]).astype(bf16).reshape(*wo_ref.shape)
    for i in range(2):
        dwo_ref[i] = r[:, i].reshape(HD // 2, D)


def out_back(o, dh, wo):
    head = pl.BlockSpec((1, T, HD), lambda i: (i, 0, 0))
    return call(out_back_body, (4,), (o, dh, wo), [head, const(T, D), pl.BlockSpec((4, *wo.shape[1:]), lambda i: (i, 0, 0, 0))],
                [head, pl.BlockSpec((1, 1, T), lambda i: (i, 0, 0)), pl.BlockSpec((2, HD // 2, D), lambda i: (0, i, 0))],
                [shape(4, T, HD), shape(4, 1, T, dtype=f32), shape(2, 2 * HD, D)], [], 4 * T * D * 4 * HD)


def attend_back_body(q_ref, k_ref, v_ref, do_ref, lse_ref, delta_ref, dq_ref, dk_ref, dv_ref, dq_s, dk_s, dv_s):
    iq = pl.program_id(0)

    @pl.when(iq == 0)
    def _():
        dk_s[:] = jnp.zeros_like(dk_s)
        dv_s[:] = jnp.zeros_like(dv_s)

    dq_s[:] = jnp.zeros_like(dq_s)

    def keys(j, masked):
        here = block(j, TILE)
        scores = [dot_t(k_ref[i, here, :], q_ref[2 * i + n]) for i, n in PIECES]
        dps = [dot_t(v_ref[i, here, :], do_ref[2 * i + n]) for i, n in PIECES]
        for m, (i, n) in enumerate(PIECES):
            p = jnp.exp2(scores[m] * EXP - lse_ref[m] * (EXP / SCALE))
            if masked:
                p = jnp.where(lax.broadcasted_iota(jnp.int32, p.shape, 1) >= lax.broadcasted_iota(jnp.int32, p.shape, 0), p, 0.0)
            ds = (p * (dps[m] - delta_ref[m])).astype(bf16)
            dv_s[i, here, :] += dot(p.astype(bf16), do_ref[m])
            dk_s[i, here, :] += dot(ds, q_ref[m])
            dq_s[m] += dot(k_ref[i, here, :].T, ds)

    lax.fori_loop(0, iq, lambda j, _: keys(j, False), None)
    keys(iq, True)
    for m in range(len(PIECES)):
        dq_ref[m] = (dq_s[m] * SCALE).T.astype(bf16)

    @pl.when(iq == pl.num_programs(0) - 1)
    def _():
        dk_ref[:] = (dk_s[:] * SCALE).astype(bf16)
        dv_ref[:] = dv_s[:].astype(bf16)


def attend_back(q, k, v, do, lse, delta):
    tile = pl.BlockSpec((4, TILE, HD), lambda i: (0, i, 0))
    stats = pl.BlockSpec((4, 1, TILE), lambda i: (0, 0, i))
    keys = const(*k.shape)
    return call(attend_back_body, (T // TILE,), (q, k, v, do, lse, delta), [tile, keys, keys, tile, stats, stats], [tile, keys, keys],
                [shape(*a.shape) for a in (q, k, v)], [pltpu.VMEM((4, HD, TILE), f32), pltpu.VMEM(k.shape, f32), pltpu.VMEM(k.shape, f32)], 10 * 2 * T * T * HD)


def qkv_back_body(dq_ref, dk_ref, dv_ref, cos_ref, sin_ref, h_ref, w_ref, dwo_ref, *rest, dx):
    dh2_ref, rest = (rest[0], rest[1:]) if dx else (None, rest)
    out_ref, wo_out, *rest = rest
    if dx:
        dh_ref, da_s, *rest = rest
    a_s, g_s, fin, xs, ls, *rest = rest
    pos = place()
    qkv, wo = Ring(pos, rest[:RING]), Ring(pos, rest[RING:])
    s = pl.program_id(0)
    slot, owner = lax.div(s, 2), lax.rem(s, 2)
    sub = 512
    pieces = [slice(m, m + sub) for m in range(0, T, sub)]
    load = pltpu.make_async_copy(dwo_ref, wo.my.at[0], ls)

    def end(slot):
        fin[:, TILE * slot : TILE * slot + TILE] = qkv.stage(slot, 4)

    @pl.when(s == 0)
    def _():
        load.start()
        greet(pos)
        for m in pieces:
            a_s[m, :] = normed(h_ref[m, :])
            if dx:
                da_s[m, :] = jnp.zeros((sub, D), f32)

    @pl.when(s == 1)
    def _():
        load.wait()
        wo.send(0)

    pl.when(s == 2)(lambda: wo.stage(0, 1))

    @pl.when(s == 3)
    def _():
        qkv.stage(0, 1)
        wo.stage(0, 2)

    def put(ref):
        for i in range(2):
            for m in pieces:
                t = ref[i, m, :]
                g_s[m, i * HD : i * HD + HD] = t if ref is dv_ref else turn(t, cos_ref[m, :], -sin_ref[m, :])

    pl.when(owner == 0)(lambda: put(dq_ref))
    pl.when(s == 1)(lambda: put(dk_ref))
    pl.when(s == 3)(lambda: put(dv_ref))
    for n in range(2):
        cols = slice(HD * n, HD * n + HD)
        qkv.my[slot, owner, :, cols] = t_dot(a_s[:], g_s[:, cols]).astype(bf16)
    pl.when(owner == 1)(lambda: qkv.send(slot))
    if dx:
        for m in pieces:
            da_s[m, :] += dot_t(g_s[m, :], w_ref[0])

    @pl.when(s == 3)
    def _():
        if dx:
            for m in pieces:
                dh_ref[m, :] = norm_back(h_ref[m, :].astype(f32), da_s[m, :], dh2_ref[m, :])

        def wo_end():
            wo_out[:] = wo.stage(0, 4)

        drain([(wo, 0, 3, wo_end), (qkv, 0, 2, lambda: end(0)), (qkv, 1, 1, lambda: end(1))])
        hand_over(pos, fin, out_ref, xs, ls)


def qkv_back(dq, dk, dv, cos, sin, h, w, dwo, dh2, cid):
    dx = dh2 is not None
    keys, rows = const(*dk.shape), D // LINES // 7
    full = [(const(T, D), shape(T, D))] if dx else []
    return pl.pallas_call(
        functools.partial(qkv_back_body, dx=dx), grid=(4,),
        in_specs=[pl.BlockSpec((2, T, HD), lambda s: (lax.div(s, 2), 0, 0)), keys, keys, const(T, HALF), const(T, HALF), const(T, D),
                  pl.BlockSpec((1, D, TILE), lambda s: (lax.rem(s, 2), 0, lax.div(s, 2))), HBM] + [spec for spec, _ in full],
        out_specs=[HBM, const(rows, D)] + [spec for spec, _ in full],
        out_shape=[shape(2, PAIR, 2 * TILE), shape(rows, D)] + [dims for _, dims in full],
        scratch_shapes=([pltpu.VMEM((T, D), f32)] if dx else []) + [pltpu.VMEM((T, D), bf16), pltpu.VMEM((T, TILE), bf16)] + hand_scratch(2 * TILE)
        + ring_scratch(PAIR, TILE) + ring_scratch(rows, D, 1),
        compiler_params=pltpu.CompilerParams(vmem_limit_bytes=LIMIT, collective_id=cid, has_side_effects=True),
        cost_estimate=pl.CostEstimate(flops=2 * T * D * 4 * TILE * (1 + dx), bytes_accessed=T * D * 10, transcendentals=0),
    )(*([dq, dk, dv, cos, sin, h, w, dwo] + ([dh2] if dx else [])))


def adamw(w, m, v, g):
    m = 0.9 * m + 0.1 * g
    v = 0.95 * v + 0.05 * g * g
    step = m * lax.rsqrt(v + 1e-8) + 0.1 * w
    return (w - 0.02 * step).astype(bf16), m, v


def tables():
    freq, fine = THETA ** (-jnp.arange(HALF, dtype=f32) / HALF), 64
    angles = [jnp.arange(n, dtype=f32)[:, None] * step * freq for n, step in ((T // fine, fine), (fine, 1))]
    return [jnp.stack([jnp.cos(a), jnp.sin(a)]) for a in angles]


def solution(mesh):
    def step(x, dy, *arrays):
        weights, m, v = (arrays[i : i + 7] for i in (0, 7, 14))
        wq, wk, wv, wo, wg, wu, wd = weights
        c = lax.rem(lax.axis_index("dp"), 2)
        pack = jnp.stack([jnp.pad(jnp.concatenate(parts, -1), ((0, 0), (0, 4), (0, 0))) for parts in ((wq, wg), (wk, wv, wu))])
        cos, sin, full, kept = forward(x[0], pack, wo, wd, *tables())
        by_h, sums = dy[0], [None, None]
        for n in (1, 0):
            h, q, k, vv, o, lse, h2, g, u, p = kept[n]
            s_gu, s_d, dh2 = ffn_back(h2, by_h, p, g, u, full[f"gu{n}"], full[f"wd{n}"], 8)
            do, delta, dwo = out_back(o, dh2, full[f"wo{n}"])
            dq, dk, dv = attend_back(q, k, vv, do, lse, delta)
            s_qkv, s_o, *rest = qkv_back(dq, dk, dv, cos, sin, h, full[f"qkv{n}"], dwo, dh2 if n else None, 9 + n)
            if n:
                by_h, = rest
            s_gu, s_qkv = (lax.dynamic_slice_in_dim(t, OWN * c, OWN, axis=1) for t in (s_gu, s_qkv))
            sums[n] = (s_qkv[0], s_qkv[1, :, :TILE], s_qkv[1, :, TILE:], s_o, s_gu[0], s_gu[1], s_d)
        gradients = [jnp.stack(pair).astype(f32) for pair in zip(*sums)]
        squares = lax.psum(sum(jnp.sum(g * g) for g in gradients), "dp")
        count = lax.psum(1, "dp") * sum(g.size for g in gradients)
        factor = jnp.minimum(1.0, 0.5 * lax.rsqrt(squares / count + 1e-30))
        new = [adamw(w.astype(f32), m, v, g * factor) for w, m, v, g in zip(weights, m, v, gradients, strict=True)]
        return tuple(one[which] for which in range(3) for one in new)

    states, cut = P(("rep", "dp"), None, None), P(None, "dp", None)
    return jax.shard_map(step, mesh=mesh, in_specs=(states, states) + (cut,) * 21, out_specs=(P("rep", "dp", None),) * 21, check_vma=False)
```

```python
import functools

import jax
import jax.numpy as jnp
from jax import lax
from jax.experimental import pallas as pl
from jax.experimental.pallas import tpu as pltpu
from jax.sharding import PartitionSpec as P

T, D, F, HD, TILE = 2048, 896, 3584, 256, 512
HALF, WIDE = HD // 2, 2 * TILE
CHIPS, LINES, CORES, HEADS = 16, 4, 2, 4
OWN = 28
PAIR = 2 * OWN
LIMIT = 67043328
f32, bf16 = jnp.float32, jnp.bfloat16
THETA = 10000
HBM = pl.BlockSpec(memory_space=pltpu.HBM)


def dot(a, b, ca=1, cb=0):
    return lax.dot_general(a, b, (((ca,), (cb,)), ((), ())), preferred_element_type=f32)


def dot_t(a, b):
    return dot(a, b, 1, 1)


def t_dot(a, b):
    return dot(a, b, 0, 0)


def rms(h):
    return lax.rsqrt(jnp.mean(h * h, -1, keepdims=True) + 1e-6)


def normed(h):
    h = h.astype(f32)
    return (h * rms(h)).astype(bf16)


def norm_back(h, db, dres):
    s = rms(h)
    m = jnp.mean(h * db, -1, keepdims=True)
    return dres + (s * db - h * (s * s * s * m)).astype(bf16)


def const(*shape):
    return pl.BlockSpec(shape, lambda *i: (0,) * len(shape), pipeline_mode=pl.Buffered(1))


def shape(*dims, dtype=bf16):
    return jax.ShapeDtypeStruct(dims, dtype)


def cut(i, n):
    return slice(i * n, i * n + n)


def along(axis, *block):
    return pl.BlockSpec(block, lambda i: tuple(i if k == axis else 0 for k in range(len(block))))


def block(at, n):
    return pl.ds(pl.multiple_of(at * n, n), n)


def place():
    me = lax.axis_index("dp")
    c, z, own = lax.rem(me, 2), lax.rem(lax.div(me, 2), LINES), lax.div(me, 2 * LINES)
    at = lambda line, z, c: (line * LINES + z) * 2 + c
    flip_x, flip_y = lax.rem(own + 2, LINES), own + 1 - 2 * lax.rem(own, 2)
    la, lb = jnp.where(c == 0, flip_y, flip_x), jnp.where(c == 0, flip_x, flip_y)
    peer = dict(d=at(own, z, 1 - c), a=at(la, z, c), b=at(lb, z, c))
    for k in range(1, LINES):
        peer[k] = at(own, lax.rem(z + k, LINES), c)
    return dict(c=c, z=z, own=own, la=la, lb=lb, ld=LINES - 1 - own, peer=peer)


def greet(pos):
    bar = pltpu.get_barrier_semaphore()
    for n in pos["peer"].values():
        pl.semaphore_signal(bar, inc=1, device_id=(0, n), device_id_type=pl.DeviceIdType.MESH)
    pl.semaphore_wait(bar, len(pos["peer"]))


def remote(src, dst, sems, i, device):
    return pltpu.make_async_remote_copy(src_ref=src, dst_ref=dst, send_sem=sems.at[0, i], recv_sem=sems.at[1, i], device_id=(0, device),
                                        device_id_type=pl.DeviceIdType.MESH)


class Gather:
    def __init__(self, pos, ref, cols, sems):
        self.pos, self.ref, self.cols, self.sems = pos, ref, cols, sems

    def part(self, chip, n):
        c = self.pos["c"]
        if len(self.ref.shape) > 3:
            return self.ref.at[pl.ds(chip, n), c]
        rows = block(chip if n == 1 else lax.div(chip, n), n * PAIR)
        return self.ref.at[c, rows] if self.cols is None else self.ref.at[c, rows, pl.ds(*self.cols)]

    def copies(self, what):
        p = self.pos
        peer, line = p["peer"], lambda name: self.part(LINES * p[name], LINES)
        mine = self.part(LINES * p["own"] + p["z"], 1)
        todo = dict(z=[(mine, k) for k in range(1, LINES)], ab=[(line("own"), "a"), (line("own"), "b")], far=[(line("la"), "b")],
                    near=[(line("own"), "d")], mid=[(line("la"), "d"), (line("lb"), "d")], last=[(line("ld"), "d")])
        first = 0
        for name, items in todo.items():
            if name == what:
                return [remote(src, src, self.sems, first + i, peer[to]) for i, (src, to) in enumerate(items)]
            first += len(items)

    def start(self, *names):
        for name in names:
            for copy in self.copies(name):
                copy.start()

    def wait(self, *names):
        for name in names:
            for copy in self.copies(name):
                copy.wait()


GATHER_SEMS = 10


PHASES = dict(z=("z",), ab=("ab", "near"), far=("far", "mid"), last=("last",))
END = 99


class Ride:
    def __init__(self, refs, plan, sems, step, last):
        self.pos, self.step, self.last = place(), step, last
        self.items = [(Gather(self.pos, refs[name], cols, sems.at[i]), phases) for i, (name, cols, phases) in enumerate(plan)]

    def do(self, phase, i, k):
        for part, phases in self.items:
            if phase in phases and phases[phase][i] == k:
                (part.wait if i else part.start)(*PHASES[phase])

    def run(self, k):
        if k < END:
            for phase in PHASES:
                self.do(phase, 1, k)
            for phase in reversed(PHASES):
                self.do(phase, 0, k)
        else:
            for phase in PHASES:
                self.do(phase, 0, k)
                self.do(phase, 1, k)

    def before(self):
        pl.when(self.step == 0)(lambda: greet(self.pos))
        for k in sorted({k for _, phases in self.items for pair in phases.values() for k in pair} - {END}):
            pl.when(self.step == k)(functools.partial(self.run, k))

    def after(self):
        pl.when(self.step == self.last)(functools.partial(self.run, END))


def call(body, grid, ins, in_specs, out_specs, outs, scratch, flops, arrays=None, plan=(), cid=None):
    names = sorted({item[0] for item in plan})
    n_in, n_out, n_scratch, n = len(ins), len(outs), len(scratch), len(names)

    def kernel(*refs):
        given, refs = refs[:n_in], refs[n_in + n :]
        made, carried, refs = refs[:n_out], refs[n_out : n_out + n], refs[n_out + n :]
        step = pl.program_id(0)
        last = grid[0] - 1
        for i, size in enumerate(grid[1:]):
            step, last = step * size + pl.program_id(i + 1), (last + 1) * size - 1
        if not plan:
            return body(*given, *made, *refs)
        ride = Ride(dict(zip(names, carried)), plan, refs[n_scratch], step, last)
        ride.before()
        body(*given, *made, *refs[:n_scratch])
        ride.after()

    extra = [arrays[name] for name in names]
    got = pl.pallas_call(
        kernel, grid=grid, in_specs=list(in_specs) + [HBM] * n, out_specs=list(out_specs) + [HBM] * n,
        out_shape=list(outs) + [shape(*a.shape) for a in extra],
        scratch_shapes=list(scratch) + ([pltpu.SemaphoreType.DMA((len(plan), 2, GATHER_SEMS))] if plan else []),
        input_output_aliases={n_in + i: n_out + i for i in range(n)},
        compiler_params=pltpu.CompilerParams(vmem_limit_bytes=LIMIT, collective_id=cid, has_side_effects=bool(plan)),
        cost_estimate=pl.CostEstimate(flops=flops, bytes_accessed=flops // 1000, transcendentals=0),
    )(*ins, *extra)
    for name, new in zip(names, got[n_out:]):
        arrays[name] = new
    return got[:n_out]


def prologue_body(pack_ref, wo_ref, wd_ref, coarse_ref, fine_ref, cos_ref, sin_ref, qkv0, qkv1, gu0, gu1, wo0, wo1, wd0, wd1, theirs, merged, xs, ls, sems):
    pos = place()
    c, me = pos["c"], LINES * pos["own"] + pos["z"]
    greet(pos)
    across = [remote(pack_ref.at[1 - c, n], theirs.at[n], xs, n, pos["peer"]["d"]) for n in range(CORES)]
    for copy in across:
        copy.start()
    local = [pltpu.make_async_copy(w.at[n], ref.at[me, c], ls.at[i, n]) for i, (w, refs) in enumerate(((wo_ref, (wo0, wo1)), (wd_ref, (wd0, wd1)))) for n, ref in enumerate(refs)]
    for copy in local:
        copy.start()

    def merge(n, first, last):
        for at in range(first, last, TILE):
            cols = slice(at, at + TILE)
            mine, other = pack_ref[c, n, :, cols].astype(f32), theirs[n, :, cols].astype(f32)
            top, low = jnp.where(c == 0, mine, other), jnp.where(c == 0, other, mine)
            both = jnp.concatenate([top, low], 0)
            moved = pltpu.roll(both, both.shape[0] - (top.shape[0] - OWN), 0)
            row = lax.broadcasted_iota(jnp.int32, both.shape, 0)
            merged[n, :, cols] = jnp.where(row < OWN, both, moved)[:PAIR].astype(bf16)

    def put(ref, n, first, size, i):
        copy = pltpu.make_async_copy(merged.at[n, :, pl.ds(first, size)], ref.at[c, block(me, PAIR)], ls.at[2 + i, n])
        copy.start()
        return copy

    halves = [Gather(pos, qkv0, (i * HD, HD), sems.at[i]) for i in range(LINES)]
    later = [Gather(pos, gu0, (F // LINES * i, F // LINES), sems.at[LINES + i]) for i in range(CORES)]
    across[0].wait()
    merge(0, 0, WIDE)
    put(qkv0, 0, 0, WIDE, 0).wait()
    for part in halves:
        part.start("z")
    merge(0, WIDE, WIDE + F)
    there = put(gu0, 0, WIDE, F, 1)
    across[1].wait()
    merge(1, 0, WIDE + F)
    rest = [there, put(qkv1, 1, 0, WIDE, 0), put(gu1, 1, WIDE, F, 1)]
    there.wait()
    for part in later:
        part.start("z")
    for part in halves:
        part.wait("z")
        part.start("ab", "near")
    fine, big = fine_ref[:], coarse_ref[:]
    n = fine.shape[1]
    for i in range(T // n):
        rows = slice(i * n, i * n + n)
        ca, sa = big[0, i : i + 1], big[1, i : i + 1]
        cos_ref[rows] = ca * fine[0] - sa * fine[1]
        sin_ref[rows] = sa * fine[0] + ca * fine[1]
    for part in halves:
        part.wait("ab")
        part.start("far", "mid")
    for part in halves:
        part.wait("far")
        part.start("last")
    for copy in local + rest[1:]:
        copy.wait()
    for part in halves:
        part.wait("near", "mid", "last")
    for part in later:
        part.wait("z")


def prologue(pack, wo, wd, coarse, fine):
    rows = pack.shape[2]
    full = [shape(CORES, D, WIDE)] * 2 + [shape(CORES, D, F)] * 2 + [shape(CHIPS, 2, wo.shape[1], D)] * 2 + [shape(CHIPS, 2, wd.shape[1], D)] * 2
    table = [shape(T, HALF, dtype=f32)] * 2
    whole = lambda a: const(*a.shape)
    got = pl.pallas_call(
        prologue_body, grid=(1,), in_specs=[whole(a) for a in (pack, wo, wd, coarse, fine)],
        out_specs=[whole(a) for a in table] + [HBM] * len(full), out_shape=table + full,
        scratch_shapes=[pltpu.VMEM((CORES, rows, pack.shape[3]), bf16), pltpu.VMEM((CORES, PAIR, pack.shape[3]), bf16), pltpu.SemaphoreType.DMA((CORES, 2)),
                        pltpu.SemaphoreType.DMA((LINES, 2)), pltpu.SemaphoreType.DMA((6, 2, GATHER_SEMS))],
        compiler_params=pltpu.CompilerParams(vmem_limit_bytes=LIMIT, collective_id=0, has_side_effects=True),
    )(pack, wo, wd, coarse, fine)
    return got[0], got[1], dict(zip(("qkv0", "qkv1", "gu0", "gu1", "wo0", "wo1", "wd0", "wd1"), got[2:]))


def turn(t, cos, sin):
    x, y = t[:, :HALF].astype(f32), t[:, HALF:].astype(f32)
    return jnp.concatenate([x * cos - y * sin, y * cos + x * sin], -1).astype(bf16)


def project_body(h_ref, w_ref, cos_ref, sin_ref, q_ref, k_ref, v_ref):
    a = normed(h_ref[:])
    cos, sin = cos_ref[:], sin_ref[:]
    for n, (owner, at, ref, head) in enumerate(((0, 0, q_ref, 0), (0, TILE, q_ref, 2), (1, 0, k_ref, 0), (1, TILE, v_ref, 0))):
        r = dot(a, w_ref[owner, :, at : at + TILE]).astype(bf16)
        for i in range(CORES):
            t = r[:, i * HD : i * HD + HD]
            ref[head + i] = turn(t, cos, sin) if ref is not v_ref else t


def project(h, w, cos, sin, *ride):
    rows = lambda width: along(0, TILE, width)
    heads = (HEADS, CORES, CORES)
    return call(project_body, (T // TILE,), (h, w, cos, sin), [rows(D), const(*w.shape), rows(HALF), rows(HALF)],
                [along(1, n, TILE, HD) for n in heads], [shape(n, T, HD) for n in heads], [], T * D * T * 2, *ride)


HIDDEN = -2e30
SCALE = HD**-0.5
EXP = SCALE * 1.4426950408889634
PIECES = [(i, n) for i in range(CORES) for n in range(CORES)]


def attend_body(q_ref, k_ref, v_ref, o_ref, lse_ref, top_s, mix_s):
    iq = pl.program_id(0)
    top_s[:] = jnp.full(top_s.shape, HIDDEN / 2, f32)
    mix_s[:] = jnp.zeros(mix_s.shape, f32)
    ones = jnp.ones((8, TILE), bf16)

    def keys(j, masked):
        here = block(j, TILE)
        scores = [dot_t(k_ref[i, here, :], q_ref[2 * i + n]) for i, n in PIECES]
        weights, keeps = [], []
        for m, s in enumerate(scores):
            if masked:
                s = jnp.where(lax.broadcasted_iota(jnp.int32, s.shape, 1) >= lax.broadcasted_iota(jnp.int32, s.shape, 0), s, HIDDEN)
            old = top_s[m : m + 1, :]
            top = jnp.maximum(old, s.max(axis=0, keepdims=True))
            top_s[m : m + 1, :] = top
            weights.append(jnp.exp2((s - top) * EXP).astype(bf16))
            keeps.append(jnp.exp2((old - top) * EXP))
        for m, (i, _) in enumerate(PIECES):
            values = jnp.concatenate([v_ref[i, here, :].T, ones], axis=0)
            mix_s[m] = mix_s[m] * keeps[m] + dot(values, weights[m])

    lax.fori_loop(0, iq, lambda j, _: keys(j, False), None)
    keys(iq, True)
    for m in range(len(PIECES)):
        total = mix_s[m, HD : HD + 1, :]
        o_ref[m] = (mix_s[m, :HD, :] * (1 / total)).T.astype(bf16)
        lse_ref[m] = top_s[m : m + 1, :] * SCALE + jnp.log(total)


def attend(q, k, v, *ride):
    tile = along(1, HEADS, TILE, HD)
    return call(attend_body, (T // TILE,), (q, k, v), [tile, const(*k.shape), const(*v.shape)],
                [tile, along(2, HEADS, 1, TILE)], [shape(HEADS, T, HD), shape(HEADS, 1, T, dtype=f32)],
                [pltpu.VMEM((HEADS, TILE), f32), pltpu.VMEM((HEADS, HD + 8, TILE), f32)], 4 * 2 * T * T * HD, *ride)


def gate_up_body(o_ref, wo_ref, h_ref, wg_ref, wu_ref, h2_ref, g_ref, u_ref, p_ref, b_s):
    j, t = pl.program_id(0), pl.program_id(1)
    tm = g_ref.shape[0]

    @pl.when(j == 0)
    def _():
        rows = block(t, tm)
        acc = sum(dot(o_ref[n, rows, :], wo_ref[4 * n : 4 * n + 4].reshape(HD, D)) for n in range(LINES))
        h2 = h_ref[rows] + acc.astype(bf16)
        h2_ref[rows] = h2
        b_s[rows] = normed(h2)

    sub = 256
    for m in range(tm // sub):
        here = cut(m, sub)
        b = b_s[block(t * (tm // sub) + m, sub), :]
        g, u = dot(b, wg_ref[0]), dot(b, wu_ref[0])
        g_ref[here] = g
        u_ref[here] = u
        p_ref[here] = (g * jax.nn.sigmoid(g) * u).astype(bf16)


def gate_up(o, wo, h, gu, *ride):
    tm = 1024
    tile = pl.BlockSpec((tm, TILE), lambda j, t: (t, j))
    weight = lambda i: pl.BlockSpec((1, D, TILE), lambda j, t: (i, 0, j))
    return call(gate_up_body, (F // TILE, T // tm), (o, wo, h, gu, gu), [const(*o.shape), const(*wo.shape), const(*h.shape), weight(0), weight(1)],
                [const(T, D), tile, tile, tile], [shape(T, D), shape(T, F, dtype=f32), shape(T, F, dtype=f32), shape(T, F)],
                [pltpu.VMEM((T, D), bf16)], 2 * T * D * (D + 2 * F), *ride)


def down_body(p_ref, wd_ref, h2_ref, h3_ref):
    acc = dot(p_ref[:], wd_ref[:])
    h3_ref[:] = h2_ref[:] + acc.astype(bf16)


def down(p, wd, h2, *ride):
    rows = lambda n: along(0, TILE, n)
    return call(down_body, (T // TILE,), (p, wd.reshape(F, D), h2), [rows(F), const(F, D), rows(D)], [rows(D)], [shape(T, D)], [], 2 * T * D * F, *ride)


PLANS = (
    dict(
        project=("gu0[0:2],ab.0.1,far.1.3,last.3.e", "gu0[2:4],ab.0.2,far.2.e,last.e.e", "gu0[4:8],z.0.e", "wo0,z.0.e"),
        attend=("wo0,ab.0.1,far.1.2,last.2.e", "gu0[4:8],ab.0.2,far.2.e,last.e.e", "wd0,z.0.e"),
        gate_up=("wd0,ab.0.5,far.5.8,last.8.e", "qkv1,z.0.5,ab.5.11,far.11.e,last.e.e", "gu1[0:2],z.5.8,ab.8.e", "gu1[2:4],z.5.e"),
        down=("gu1[0:2],far.0.e", "gu1[2:4],ab.0.e", "gu1[4:6],z.0.e"),
    ),
    dict(
        project=("gu1[0:2],last.0.e", "gu1[2:4],far.0.e", "gu1[4:6],ab.0.e", "gu1[6:8],z.0.e", "wo1,z.0.e"),
        attend=("gu1[2:4],last.0.e", "gu1[4:6],far.0.3,last.3.e", "gu1[6:8],ab.0.3,far.3.e,last.e.e", "wo1,ab.0.3,far.3.e,last.e.e", "wd1,z.0.e"),
        gate_up=("wd1,ab.0.6,far.6.10,last.10.e",),
    ),
)


def read_plan(text):
    name, *todo = text.split(",")
    name, _, cols = name.rstrip("]").partition("[")
    if cols:
        first, end = (F // 8 * int(n) for n in cols.split(":"))
        cols = (first, end - first)
    phases = [item.split(".") for item in todo]
    return name, cols or None, {phase: [END if k == "e" else int(k) for k in steps] for phase, *steps in phases}


def forward(x, pack, wo, wd, coarse, fine):
    cos, sin, arrays = prologue(pack, wo, wd, coarse, fine)
    h, kept, cid = x, [], 1
    for n, texts in enumerate(PLANS):
        plan = {name: [read_plan(item) for item in text] for name, text in texts.items()}
        q, k, v = project(h, arrays[f"qkv{n}"], cos, sin, arrays, plan["project"], cid)
        o, lse = attend(q, k, v, arrays, plan["attend"], cid + 1)
        h2, g, u, p = gate_up(o, arrays[f"wo{n}"], h, arrays[f"gu{n}"], arrays, plan["gate_up"], cid + 2)
        kept.append((h, q, k, v, o, lse, h2, g, u, p))
        if n == 0:
            h, = down(p, arrays["wd0"], h2, arrays, plan["down"], cid + 3)
        cid += 4
    return cos, sin, arrays, kept


def ring_scratch(rows, width, slots=2):
    line = LINES * rows
    dims = ((2, LINES * line), (LINES * line,), (2, line), (line,), (LINES, rows), (LINES - 1, rows))
    return [pltpu.VMEM((slots, *d, width), bf16) for d in dims] + [pltpu.SemaphoreType.DMA((slots, 2, 7))]


RING = 7


class Ring:
    def __init__(self, pos, refs):
        self.pos = pos
        self.my, self.rd, self.rb, self.ra, self.zs, self.rz, self.sems = refs
        self.rows = self.zs.shape[2]

    def line(self, l):
        return block(l, LINES * self.rows)

    def copies(self, slot, stage, source=None):
        p, peer, sems = self.pos, self.pos["peer"], self.sems.at[slot]
        mine = self.my.at[slot, p["c"]]
        if stage == 0:
            source = self.my.at[slot] if source is None else source
            return [remote(source.at[1 - p["c"]], self.rd.at[slot], sems, 0, peer["d"])]
        if stage == 1:
            return [remote(mine.at[self.line(p[name])], self.rb.at[slot, i], sems, 1 + i, peer["b"]) for i, name in enumerate(("lb", "ld"))]
        if stage == 2:
            return [remote(mine.at[self.line(p["la"])], self.ra.at[slot], sems, 3, peer["a"])]
        return [remote(self.zs.at[slot, lax.rem(p["z"] + k, LINES)], self.rz.at[slot, k - 1], sems, 3 + k, peer[k]) for k in range(1, LINES)]

    def send(self, slot, stage=0, source=None):
        for copy in self.copies(slot, stage, source):
            copy.start()

    def add(self, slot, l, theirs):
        n, size = LINES * self.rows, 32
        c = self.pos["c"]

        def some(i, _):
            here, there = pl.ds(pl.multiple_of(n * l + i * size, size), size), pl.ds(pl.multiple_of(i * size, size), size)
            self.my[slot, c, here, :] = (self.my[slot, c, here, :].astype(f32) + theirs[there, :].astype(f32)).astype(bf16)

        lax.fori_loop(0, n // size, some, None)

    def stage(self, slot, n):
        p = self.pos
        for copy in self.copies(slot, n - 1):
            copy.wait()
        if n == 1:
            for l in range(LINES):
                self.add(slot, l, self.rd.at[slot, self.line(l)])
        elif n == 2:
            self.add(slot, p["own"], self.rb.at[slot, 0])
            self.add(slot, p["la"], self.rb.at[slot, 1])
        elif n == 3:
            mine = self.my[slot, p["c"], self.line(p["own"]), :].astype(f32)
            self.zs[slot] = (mine + self.ra[slot].astype(f32)).reshape(LINES, self.rows, -1).astype(bf16)
        else:
            return (self.zs[slot, p["z"]].astype(f32) + sum(self.rz[slot, k].astype(f32) for k in range(LINES - 1))).astype(bf16)
        self.send(slot, n)


def drain(units):
    while units:
        for ring, slot, n, end in units:
            ring.stage(slot, n) if n < 4 else end()
        units = [(ring, slot, n + 1, end) for ring, slot, n, end in units if n < 4]


def finish(copies):
    for copy in copies:
        copy.wait()


def ffn_back_body(h2_ref, dy_ref, p_ref, g_ref, u_ref, wg_ref, wu_ref, wd_ref, o_ref, wo_ref, fin, late_out, wd_out, dh_ref, do_ref, dwo_ref,
                  b_s, db_s, dg_s, du_s, ls, *rest):
    j, t = pl.program_id(0), pl.program_id(1)
    tm, nj, nt = g_ref.shape[0], pl.num_programs(0) - 1, pl.num_programs(1) - 1
    pos = place()
    gu, wd = Ring(pos, rest[:RING]), Ring(pos, rest[RING:])
    slot, old = lax.rem(j, 2), lax.rem(j + 1, 2)
    third = lambda n: lax.rem(n, 3)
    at = lambda k, *also: functools.partial(pl.when, functools.reduce(lambda a, b: a & b, also, t == k))()
    at(0, j == 0)(lambda: greet(pos))
    sub = 256
    n_last = F // TILE - 1
    more, both, ours, late = j >= 1, j >= 2, (j >= 1) & (j < nj), j == nj - 1

    def gu_end():
        fin[:, block(j - 2, TILE)] = gu.stage(slot, 4)

    def wd_end(j):
        wd_out[:, block(j, HALF)] = wd.stage(third(j), 4)

    at(0, both)(lambda: wd_end(j - 2))
    at(0, both)(lambda: gu.stage(slot, 3))
    at(0, more)(lambda: wd.stage(third(j + 2), 1))
    at(1, ours)(lambda: gu.stage(old, 1))
    at(2, more)(lambda: wd.stage(third(j + 2), 2))
    at(3, both)(gu_end)
    at(3, j == nj)(lambda: wd.stage(third(j + 2), 3))

    @at(4, ours)
    def _():
        gu.stage(old, 2)
        wd.stage(third(j + 2), 3)

    @pl.when((t < nt) & (j < nj))
    def _():
        rows = block(t, tm)

        @pl.when(j == 0)
        def _():
            b_s[rows] = normed(h2_ref[rows])
            db_s[rows] = jnp.zeros((tm, D), f32)

        for m in range(tm // sub):
            here, rows = cut(m, sub), block(t * (tm // sub) + m, sub)
            dp = dot_t(dy_ref[rows], wd_ref[:]).astype(bf16).astype(f32)
            g, u = g_ref[here], u_ref[here]
            s = jax.nn.sigmoid(g)
            gs = g * s
            du = (dp * gs).astype(bf16)
            dg = (dp * u * (s + gs * (1 - s))).astype(bf16)
            dg_s[rows] = dg
            du_s[rows] = du
            db_s[rows] += dot_t(dg, wg_ref[0]) + dot_t(du, wu_ref[0])

        for n in range(LINES):
            width, rows = min(sub, D - sub * n), wd.rows

            @pl.when(j == 2 * n)
            def _():
                r = t_dot(p_ref[:], dy_ref[:, sub * n : sub * n + width]).astype(bf16)
                for q in range(8):
                    at = pl.multiple_of(LINES * rows * t + rows * (q // 2), rows)
                    for e in range(width // HALF):
                        wd.my[(2 * n + e) % 3, q % 2, pl.ds(at, rows), :] = r[rows * q : rows * q + rows, HALF * e : HALF * e + HALF]

        @pl.when(late)
        def _():
            for m in range(tm // sub):
                rows = block(t * (tm // sub) + m, sub)
                dh_ref[rows] = norm_back(h2_ref[rows].astype(f32), db_s[rows], dy_ref[rows])

    at(3, j < nj)(lambda: wd.send(third(j)))

    @at(4, j < nj)
    def _():
        for i, ref in enumerate((dg_s, du_s)):
            for n in range(TILE // sub):
                cols = cut(n, sub)
                gu.my[slot, i, :, cols] = t_dot(b_s[:], ref[:, cols]).astype(bf16)
        pl.when(j < nj - 1)(lambda: gu.send(slot))

    save = pltpu.make_async_copy(gu.my.at[n_last % 2], late_out, ls)
    at(4, late)(lambda: save.start())

    @pl.when((j == nj) & (t < nt))
    def _():
        do_ref[0] = dot_t(dh_ref[:], wo_ref[:].reshape(HD, D)).astype(bf16)
        r = t_dot(o_ref[0], dh_ref[:]).astype(bf16).reshape(*wo_ref.shape)
        for i in range(CORES):
            dwo_ref[i] = r[:, i].reshape(HALF, D)

    @at(4, j == nj)
    def _():
        wd_end(n_last)
        save.wait()


def ffn_back(h2, dy, p, g, u, gu, wd, o, wo, cid):
    tm = 512
    nj, nt = F // TILE, T // tm
    wide = D
    tj = lambda j: jnp.minimum(j, nj - 1)
    tt = lambda j, t: jnp.where(j < nj, jnp.minimum(t, nt - 1), nt - 1)
    head = lambda j, t: jnp.where(j < nj, 0, jnp.minimum(t, nt - 1))
    weight = lambda i: pl.BlockSpec((1, D, TILE), lambda j, t: (i, 0, tj(j)))
    tile = pl.BlockSpec((tm, TILE), lambda j, t: (tt(j, t), tj(j)))
    one = pl.BlockSpec((1, T, HD), lambda j, t: (head(j, t), 0, 0))
    rows, done = F // CHIPS // 2, F - TILE
    return pl.pallas_call(
        ffn_back_body, grid=(nj + 1, nt + 1),
        in_specs=[const(T, D), const(T, D), pl.BlockSpec((T, wide), lambda j, t: (0, jnp.where(lax.rem(j, 2) == 0, tt(j, t), nt - 1))), tile, tile,
                  weight(0), weight(1), pl.BlockSpec((TILE, D), lambda j, t: (tj(j), 0)), one,
                  pl.BlockSpec((4, *wo.shape[1:]), lambda j, t: (head(j, t), 0, 0, 0))],
        out_specs=[const(PAIR, done), HBM, const(rows, D), const(T, D), one, pl.BlockSpec((CORES, HALF, D), lambda j, t: (0, head(j, t), 0))],
        out_shape=[shape(PAIR, done), shape(CORES, D, TILE), shape(rows, D), shape(T, D), shape(HEADS, T, HD), shape(CORES, TILE, D)],
        scratch_shapes=[pltpu.VMEM((T, D), bf16), pltpu.VMEM((T, D), f32), pltpu.VMEM((T, TILE), bf16), pltpu.VMEM((T, TILE), bf16)]
        + [pltpu.SemaphoreType.DMA(())] + ring_scratch(PAIR, TILE) + ring_scratch(rows, HALF, 3),
        compiler_params=pltpu.CompilerParams(vmem_limit_bytes=LIMIT, collective_id=cid, has_side_effects=True),
        cost_estimate=pl.CostEstimate(flops=12 * T * D * F, bytes_accessed=F * T * 12, transcendentals=0),
    )(h2, dy, p, g, u, gu, gu, wd.reshape(F, D), o, wo)


DUE = ((4, 6), (6, 8), (7, 8), (8,))


def attend_back_body(q_ref, k_ref, v_ref, do_ref, o_ref, lse_ref, wo_in, *refs, units):
    given, refs = refs[:units], refs[units:]
    dq_ref, dk_ref, dv_ref, wo_out, fin, dq_s, dk_s, dv_s, delta_s, loads, *rest = refs
    iq = pl.program_id(0)
    pos = place()
    wide, wo = Ring(pos, rest[:RING]), Ring(pos, rest[RING:])
    todo = [(wide, 0, given[0]), (wo, 0, wo_in)] + [(wide, 1 + i, ref.at[i]) for ref in given[1:] for i in range(CORES)]
    mine = [pltpu.make_async_copy(ref.at[pos["c"]], ring.my.at[slot, pos["c"]], loads.at[i]) for i, (ring, slot, ref) in enumerate(todo)]

    def end(ring, slot):
        if ring is wo:
            wo_out[:] = ring.stage(slot, 4)
        else:
            fin[:, TILE * slot : TILE * slot + TILE] = ring.stage(slot, 4)

    def event(e):
        @pl.when(e == 1)
        def _():
            for copy, (ring, slot, _) in zip(mine, todo):
                copy.wait()
                ring.stage(slot, 1)

        for (ring, slot, _), steps in zip(todo, DUE):
            for n, k in enumerate(steps):
                pl.when(e == k)(functools.partial(ring.stage, slot, n + 2))

    @pl.when(iq == 0)
    def _():
        for copy in mine:
            copy.start()
        greet(pos)
        for ring, slot, ref in todo:
            ring.send(slot, 0, ref)
        dk_s[:] = jnp.zeros_like(dk_s)
        dv_s[:] = jnp.zeros_like(dv_s)

    dq_s[:] = jnp.zeros_like(dq_s)
    for m in range(len(PIECES)):
        x = do_ref[m].astype(f32) * o_ref[m].astype(f32)
        delta_s[m] = (x[:, :HALF] + x[:, HALF:]).T.sum(axis=0, keepdims=True)

    def keys(j, masked):
        here = block(j, TILE)
        scores = [dot_t(k_ref[i, here, :], q_ref[2 * i + n]) for i, n in PIECES]
        dps = [dot_t(v_ref[i, here, :], do_ref[2 * i + n]) for i, n in PIECES]
        for m, (i, n) in enumerate(PIECES):
            p = jnp.exp2(scores[m] * EXP - lse_ref[m] * (EXP / SCALE))
            if masked:
                p = jnp.where(lax.broadcasted_iota(jnp.int32, p.shape, 1) >= lax.broadcasted_iota(jnp.int32, p.shape, 0), p, 0.0)
            ds = (p * (dps[m] - delta_s[m])).astype(bf16)
            dv_s[i, here, :] += dot(p.astype(bf16), do_ref[m])
            dk_s[i, here, :] += dot(ds, q_ref[m])
            dq_s[m] += dot(k_ref[i, here, :].T, ds)

    @functools.partial(lax.fori_loop, 0, iq, init_val=None)
    def _(j, _):
        event(lax.div(iq * (iq + 1), 2) + j)
        keys(j, False)

    keys(iq, True)
    for m in range(len(PIECES)):
        dq_ref[m] = (dq_s[m] * SCALE).T.astype(bf16)

    @pl.when(iq == pl.num_programs(0) - 1)
    def _():
        dk_ref[:] = (dk_s[:] * SCALE).astype(bf16)
        dv_ref[:] = dv_s[:].astype(bf16)
        drain([(ring, slot, 2 + len(steps), functools.partial(end, ring, slot)) for (ring, slot, _), steps in zip(todo, DUE)])


def attend_back(q, k, v, do, o, lse, dwo, units, cid):
    tile = along(1, HEADS, TILE, HD)
    keys, rows, n = const(*k.shape), D // OWN, len(units)
    n_wide = CORES * n - 1
    return pl.pallas_call(
        functools.partial(attend_back_body, units=n), grid=(T // TILE,),
        in_specs=[tile, keys, keys, tile, tile, along(2, HEADS, 1, TILE)] + [HBM] * (1 + n),
        out_specs=[tile, keys, keys, const(rows, D), const(PAIR, n_wide * TILE)],
        out_shape=[shape(*a.shape) for a in (q, k, v)] + [shape(rows, D), shape(PAIR, n_wide * TILE)],
        scratch_shapes=[pltpu.VMEM((HEADS, HD, TILE), f32), pltpu.VMEM(k.shape, f32), pltpu.VMEM(k.shape, f32), pltpu.VMEM((HEADS, 1, TILE), f32)]
        + [pltpu.SemaphoreType.DMA((1 + n_wide,))] + ring_scratch(PAIR, TILE, n_wide) + ring_scratch(rows, D, 1),
        compiler_params=pltpu.CompilerParams(vmem_limit_bytes=LIMIT, collective_id=cid, has_side_effects=True),
        cost_estimate=pl.CostEstimate(flops=20 * T * T * HD, bytes_accessed=T * D * 12, transcendentals=0),
    )(q, k, v, do, o, lse, dwo, *units)


def turn_back(ref, g_s, first, *angles):
    sub = 512
    for i in range(ref.shape[0]):
        at = first + i * HD
        for m in range(0, T, sub):
            rows = slice(m, m + sub)
            t = ref[i, rows, :]
            g_s[rows, at : at + HD] = turn(t, angles[0][rows], -angles[1][rows]) if angles else t


def qkv_back_body(dq_ref, dk_ref, dv_ref, cos_ref, sin_ref, h_ref, w_ref, dh2_ref, dw_ref, dh_ref, a_s, g_s, da_s):
    s = pl.program_id(0)
    sub = 512
    pieces = [slice(m, m + sub) for m in range(0, T, sub)]

    @pl.when(s == 0)
    def _():
        for m in pieces:
            a_s[m] = normed(h_ref[m])
            da_s[m] = jnp.zeros((sub, D), f32)

    for k, ref in enumerate((dq_ref, dk_ref, dq_ref, dv_ref)):
        angles = () if ref is dv_ref else (cos_ref, sin_ref)
        pl.when(s == k)(functools.partial(turn_back, ref, g_s, 0, *angles))
    dw_ref[0, 0] = t_dot(a_s[:], g_s[:]).astype(bf16)
    for m in pieces:
        da_s[m] += dot_t(g_s[m], w_ref[0])

    @pl.when(s == 3)
    def _():
        for m in pieces:
            dh_ref[m] = norm_back(h_ref[m].astype(f32), da_s[m], dh2_ref[m])


def qkv_back(dq, dk, dv, cos, sin, h, w, dh2):
    keys = const(*dk.shape)
    return call(qkv_back_body, (HEADS,), (dq, dk, dv, cos, sin, h, w, dh2),
                [pl.BlockSpec((CORES, T, HD), lambda s: (lax.div(s, 2), 0, 0)), keys, keys, const(T, HALF), const(T, HALF), const(T, D),
                 pl.BlockSpec((1, D, TILE), lambda s: (lax.rem(s, 2), 0, lax.div(s, 2))), const(T, D)],
                [pl.BlockSpec((1, 1, D, TILE), lambda s: (lax.div(s, 2), lax.rem(s, 2), 0, 0)), const(T, D)], [shape(CORES, 2, D, TILE), shape(T, D)],
                [pltpu.VMEM((T, D), bf16), pltpu.VMEM((T, TILE), bf16), pltpu.VMEM((T, D), f32)], 4 * T * D * 4 * TILE)


def qkv_last_body(dq_ref, dk_ref, dv_ref, cos_ref, sin_ref, h_ref, fin, a_s, g_s, *rest):
    pos = place()
    ring = Ring(pos, rest)
    s = pl.program_id(0)

    @pl.when(s == 0)
    def _():
        greet(pos)
        a_s[:] = normed(h_ref[:])

    turn_back(dq_ref, g_s, 0, cos_ref, sin_ref)
    pl.when(s < 2)(lambda: turn_back(dk_ref, g_s, HD, cos_ref, sin_ref))
    pl.when(s >= 2)(lambda: turn_back(dv_ref, g_s, HD))
    for i in range(CORES):
        ring.my[s, i] = t_dot(a_s[:], g_s[:, HD * i : HD * i + HD]).astype(bf16)
    ring.send(s)

    def end(slot):
        fin[:, HD * slot : HD * slot + HD] = ring.stage(slot, 4)

    for k in range(1, 4):
        for n in range(1, k + 1):
            pl.when(s == k)(functools.partial(ring.stage, k - n, n))

    @pl.when(s == 3)
    def _():
        drain([(ring, slot, 4 - slot, functools.partial(end, slot)) for slot in range(LINES)])


def qkv_last(dq, dk, dv, cos, sin, h, cid):
    head = lambda n, of: pl.BlockSpec((1, T, HD), lambda s: (jnp.clip(s - n, 0, of - 1), 0, 0))
    return pl.pallas_call(
        qkv_last_body, grid=(HEADS,), in_specs=[head(0, 4), head(0, 2), head(2, 2), const(T, HALF), const(T, HALF), const(T, D)], out_specs=const(PAIR, WIDE),
        out_shape=shape(PAIR, WIDE),
        scratch_shapes=[pltpu.VMEM((T, D), bf16), pltpu.VMEM((T, TILE), bf16)] + ring_scratch(PAIR, HD, 4),
        compiler_params=pltpu.CompilerParams(vmem_limit_bytes=LIMIT, collective_id=cid, has_side_effects=True),
        cost_estimate=pl.CostEstimate(flops=2 * T * D * 4 * TILE, bytes_accessed=T * D * 10, transcendentals=0),
    )(dq, dk, dv, cos, sin, h)


def sources(gu, late, qkv, first):
    wide = F - TILE
    pair = lambda owner: [(gu, owner, 0, 0, wide), (late, owner, 0, wide, TILE)]
    return [[(qkv, 0, first, 0, WIDE)], [(qkv, 1, first, 0, TILE)], [(qkv, 1, first + TILE, 0, TILE)], pair(0), pair(1)]


def own_rows(c, both, owner, cols):
    mine, theirs = (ref[:, cols].astype(f32) for ref in both)
    x = jnp.where(c == owner, mine, theirs)
    return jnp.where(c == 0, x, pltpu.roll(x, OWN, 0))[:OWN]


def lay_out(c, pairs, outs):
    gu0, late0, last0, gu1, late1 = pairs
    for n, from_layer in enumerate((sources(gu0, late0, last0, 0), sources(gu1, late1, late0, TILE))):
        for out, parts in zip(outs, from_layer):
            for ref, owner, at, to, width in parts:
                for k in range(0, width, TILE):
                    out[:, n, to + k : to + k + TILE] = own_rows(c, ref, owner, slice(at + k, at + k + TILE))


def squares_body(*refs, n_sums, n_halved):
    sums, out_ref, grads = refs[:n_sums], refs[n_sums], refs[n_sums + 1 : -4 - n_halved]
    *others, mine, parts, swap, sems = refs[-4 - n_halved :]
    pos = place()
    greet(pos)
    halved = sums[:n_halved]
    across = [remote(ref, other, swap, i, pos["peer"]["d"]) for i, (ref, other) in enumerate(zip(halved, others))]
    for copy in across:
        copy.start()
    total = jnp.zeros((1, HALF), f32)
    for ref in sums:
        for at in range(0, ref.shape[1], HALF):
            x = ref[:, at : at + HALF].astype(f32)
            total += (x * x).sum(axis=0, keepdims=True)
    mine[:] = jnp.broadcast_to(total, mine.shape)
    n = 0
    for names in ("d", "a", "b", range(1, LINES)):
        copies = [remote(mine, parts.at[n + i], sems, n + i, pos["peer"][name]) for i, name in enumerate(names)]
        for copy in copies:
            copy.start()
        if n == 1:
            finish(across)
            lay_out(pos["c"], list(zip(halved, others)), grads)
        finish(copies)
        mine[:] += sum(parts[n + i] for i in range(len(names)))
        n += len(names)
    out_ref[:] = mine[:]


def squares(halved, whole, cid):
    part, peers, sums = (8, HALF), LINES + 2, (*halved, *whole)
    outs = [shape(*part, dtype=f32)] + [shape(OWN, 2, n, dtype=f32) for n in (WIDE, TILE, TILE, F, F)]
    return pl.pallas_call(
        functools.partial(squares_body, n_sums=len(sums), n_halved=len(halved)), grid=(1,), in_specs=[const(*a.shape) for a in sums],
        out_specs=[const(*a.shape) for a in outs], out_shape=outs,
        scratch_shapes=[pltpu.VMEM(a.shape, bf16) for a in halved]
        + [pltpu.VMEM(part, f32), pltpu.VMEM((peers, *part), f32), pltpu.SemaphoreType.DMA((CORES, len(halved))), pltpu.SemaphoreType.DMA((CORES, peers))],
        compiler_params=pltpu.CompilerParams(vmem_limit_bytes=LIMIT, collective_id=cid, has_side_effects=True),
    )(*sums)


def adamw(w, m, v, g):
    m = 0.9 * m + 0.1 * g
    v = 0.95 * v + 0.05 * g * g
    step = m * lax.rsqrt(v + 1e-8) + 0.1 * w
    return (w - 0.02 * step).astype(bf16), m, v


def update(halved, whole, weights, m, v, cid):
    total, *grads = squares(halved, whole, cid)
    count = 2 * CHIPS * sum(w.size for w in weights)
    factor = jnp.minimum(1.0, 0.5 * lax.rsqrt(total[0].sum() / count + 1e-30))
    q, k, vv, gate, up = (g.transpose(1, 0, 2) for g in grads)
    o0, d0, o1, d1 = whole
    both = lambda *layers: jnp.stack(layers).astype(f32)
    grads = q, k, vv, both(o0, o1), gate, up, both(d0, d1)
    new = [adamw(w.astype(f32), m, v, g * factor) for w, m, v, g in zip(weights, m, v, grads, strict=True)]
    return tuple(one[which] for which in range(3) for one in new)


def tables():
    freq, fine = THETA ** (-jnp.arange(HALF, dtype=f32) / HALF), 64
    angles = [jnp.arange(n, dtype=f32)[:, None] * step * freq for n, step in ((T // fine, fine), (fine, 1))]
    return [jnp.stack([jnp.cos(a), jnp.sin(a)]) for a in angles]


def solution(mesh):
    def step(x, dy, *arrays):
        wq, wk, wv, wo, wg, wu, wd = arrays[:7]
        pack = jnp.stack([jnp.pad(jnp.concatenate(parts, -1), ((0, 0), (0, 4), (0, 0))) for parts in ((wq, wg), (wk, wv, wu))])
        cos, sin, full, kept = forward(x[0], pack, wo, wd, *tables())
        by_h, late, halved, whole = dy[0], [], [], []
        for n in (1, 0):
            h, q, k, vv, o, lse, h2, g, u, p = kept[n]
            s_gu, last, s_d, dh2, do, dwo = ffn_back(h2, by_h, p, g, u, full[f"gu{n}"], full[f"wd{n}"], o, full[f"wo{n}"], 8)
            dq, dk, dv, s_o, s_late = attend_back(q, k, vv, do, o, lse, dwo, [last, *late], 9 + n)
            if n:
                dqkv, by_h = qkv_back(dq, dk, dv, cos, sin, h, full[f"qkv{n}"], dh2)
                late = [dqkv]
            last = [] if n else [qkv_last(dq, dk, dv, cos, sin, h, 11)]
            halved, whole = [s_gu, s_late, *last, *halved], [s_o, s_d, *whole]
        return update(halved, whole, *(arrays[i : i + 7] for i in (0, 7, 14)), 12)

    states, cut = P(("rep", "dp")), P(None, "dp")
    return jax.shard_map(step, mesh=mesh, in_specs=(states, states) + (cut,) * 21, out_specs=(P("rep", "dp"),) * 21, check_vma=False)
```

```python
import functools

import jax
import jax.numpy as jnp
from jax import lax
from jax.experimental import pallas as pl
from jax.experimental.pallas import tpu as pltpu
from jax.sharding import PartitionSpec as P

T, D, F, HD, TILE = 2048, 896, 3584, 256, 512
HALF, WIDE = HD // 2, 2 * TILE
CHIPS, LINES, CORES, HEADS = 16, 4, 2, 4
OWN = 28
PAIR = 2 * OWN
LIMIT = 67043328
f32, bf16 = jnp.float32, jnp.bfloat16
THETA = 10000
HBM = pl.BlockSpec(memory_space=pltpu.HBM)


def dot(a, b, ca=1, cb=0):
    return lax.dot_general(a, b, (((ca,), (cb,)), ((), ())), preferred_element_type=f32)


def dot_t(a, b):
    return dot(a, b, 1, 1)


def t_dot(a, b):
    return dot(a, b, 0, 0)


def rms(h):
    return lax.rsqrt(jnp.mean(h * h, -1, keepdims=True) + 1e-6)


def normed(h):
    h = h.astype(f32)
    return (h * rms(h)).astype(bf16)


def norm_back(h, db, dres):
    s = rms(h)
    m = jnp.mean(h * db, -1, keepdims=True)
    return dres + (s * db - h * (s * s * s * m)).astype(bf16)


def const(*shape):
    return pl.BlockSpec(shape, lambda *i: (0,) * len(shape), pipeline_mode=pl.Buffered(1))


def shape(*dims, dtype=bf16):
    return jax.ShapeDtypeStruct(dims, dtype)


def cut(i, n):
    return slice(i * n, i * n + n)


def along(axis, *block):
    return pl.BlockSpec(block, lambda i: tuple(i if k == axis else 0 for k in range(len(block))))


def block(at, n):
    return pl.ds(pl.multiple_of(at * n, n), n)


def place():
    me = lax.axis_index("dp")
    c, z, own = lax.rem(me, CORES), lax.rem(lax.div(me, CORES), LINES), lax.div(me, CORES * LINES)
    at = lambda line, z, c: (line * LINES + z) * CORES + c
    flip_x, flip_y = lax.rem(own + 2, LINES), own + 1 - 2 * lax.rem(own, 2)
    la, lb = jnp.where(c == 0, flip_y, flip_x), jnp.where(c == 0, flip_x, flip_y)
    peer = dict(d=at(own, z, 1 - c), a=at(la, z, c), b=at(lb, z, c))
    for k in range(1, LINES):
        peer[k] = at(own, lax.rem(z + k, LINES), c)
    return dict(c=c, z=z, own=own, la=la, lb=lb, ld=LINES - 1 - own, peer=peer)


def greet(pos):
    bar = pltpu.get_barrier_semaphore()
    for n in pos["peer"].values():
        pl.semaphore_signal(bar, inc=1, device_id=(0, n), device_id_type=pl.DeviceIdType.MESH)
    pl.semaphore_wait(bar, len(pos["peer"]))


def remote(src, dst, sems, i, device):
    return pltpu.make_async_remote_copy(src_ref=src, dst_ref=dst, send_sem=sems.at[0, i], recv_sem=sems.at[1, i], device_id=(0, device),
                                        device_id_type=pl.DeviceIdType.MESH)


class Gather:
    def __init__(self, pos, ref, cols, sems):
        self.pos, self.ref, self.cols, self.sems = pos, ref, cols, sems

    def part(self, chip, n):
        c = self.pos["c"]
        if len(self.ref.shape) > 3:
            return self.ref.at[pl.ds(chip, n), c]
        rows = block(chip if n == 1 else lax.div(chip, n), n * PAIR)
        return self.ref.at[c, rows, pl.ds(*self.cols)] if self.cols else self.ref.at[c, rows]

    def copies(self, what):
        p = self.pos
        peer, line = p["peer"], lambda name: self.part(LINES * p[name], LINES)
        mine = self.part(LINES * p["own"] + p["z"], 1)
        todo = dict(z=[(mine, k) for k in range(1, LINES)], ab=[(line("own"), "a"), (line("own"), "b")], far=[(line("la"), "b")],
                    near=[(line("own"), "d")], mid=[(line("la"), "d"), (line("lb"), "d")], last=[(line("ld"), "d")])
        first = 0
        for name, items in todo.items():
            if name == what:
                return [remote(src, src, self.sems, first + i, peer[to]) for i, (src, to) in enumerate(items)]
            first += len(items)

    def start(self, *names):
        for name in names:
            for copy in self.copies(name):
                copy.start()

    def wait(self, *names):
        for name in names:
            for copy in self.copies(name):
                copy.wait()


GATHER_SEMS = 10


PHASES = dict(z=("z",), ab=("ab", "near"), far=("far", "mid"), last=("last",))
END = 99


class Ride:
    def __init__(self, refs, plan, sems, step, last):
        self.pos, self.step, self.last = place(), step, last
        self.items = [(Gather(self.pos, refs[name], cols, sems.at[i]), phases) for i, (name, cols, phases) in enumerate(plan)]

    def do(self, phase, i, k):
        for part, phases in self.items:
            if phase in phases and phases[phase][i] == k:
                (part.wait if i else part.start)(*PHASES[phase])

    def run(self, k):
        if k < END:
            for phase in PHASES:
                self.do(phase, 1, k)
            for phase in reversed(PHASES):
                self.do(phase, 0, k)
        else:
            for phase in PHASES:
                self.do(phase, 0, k)
                self.do(phase, 1, k)

    def before(self):
        pl.when(self.step == 0)(lambda: greet(self.pos))
        for k in sorted({k for _, phases in self.items for pair in phases.values() for k in pair} - {END}):
            pl.when(self.step == k)(functools.partial(self.run, k))

    def after(self):
        pl.when(self.step == self.last)(functools.partial(self.run, END))


def call(body, grid, ins, in_specs, out_specs, outs, scratch, flops, arrays=(), plan=(), cid=None):
    names = sorted({item[0] for item in plan})
    n_in, n_out, n_scratch, n = len(ins), len(outs), len(scratch), len(names)

    def kernel(*refs):
        given, refs = refs[:n_in], refs[n_in + n :]
        made, carried, refs = refs[:n_out], refs[n_out : n_out + n], refs[n_out + n :]
        step = pl.program_id(0)
        last = grid[0] - 1
        for i, size in enumerate(grid[1:]):
            step, last = step * size + pl.program_id(i + 1), (last + 1) * size - 1
        if not plan:
            return body(*given, *made, *refs)
        ride = Ride(dict(zip(names, carried)), plan, refs[n_scratch], step, last)
        ride.before()
        body(*given, *made, *refs[:n_scratch])
        ride.after()

    extra = [arrays[name] for name in names]
    got = pl.pallas_call(
        kernel, grid=grid, in_specs=list(in_specs) + [HBM] * n, out_specs=list(out_specs) + [HBM] * n,
        out_shape=list(outs) + [shape(*a.shape) for a in extra],
        scratch_shapes=list(scratch) + ([pltpu.SemaphoreType.DMA((len(plan), 2, GATHER_SEMS))] if plan else []),
        input_output_aliases={n_in + i: n_out + i for i in range(n)},
        compiler_params=pltpu.CompilerParams(vmem_limit_bytes=LIMIT, collective_id=cid, has_side_effects=bool(plan)),
        cost_estimate=pl.CostEstimate(flops=flops, bytes_accessed=flops // 1000, transcendentals=0),
    )(*ins, *extra)
    for name, new in zip(names, got[n_out:]):
        arrays[name] = new
    return got[:n_out]


def prologue_body(pack_ref, wo_ref, wd_ref, coarse_ref, fine_ref, cos_ref, sin_ref, qkv0, qkv1, gu0, gu1, wo0, wo1, wd0, wd1, theirs, merged, xs, ls, sems):
    pos = place()
    c, me = pos["c"], LINES * pos["own"] + pos["z"]
    greet(pos)
    across = [remote(pack_ref.at[1 - c, n], theirs.at[n], xs, n, pos["peer"]["d"]) for n in range(CORES)]
    for copy in across:
        copy.start()
    local = [pltpu.make_async_copy(w.at[n], ref.at[me, c], ls.at[i, n]) for i, (w, refs) in enumerate(((wo_ref, (wo0, wo1)), (wd_ref, (wd0, wd1)))) for n, ref in enumerate(refs)]
    for copy in local:
        copy.start()

    def merge(n, first, last):
        for at in range(first, last, TILE):
            cols = slice(at, at + TILE)
            mine, other = pack_ref[c, n, :, cols].astype(f32), theirs[n, :, cols].astype(f32)
            top, low = jnp.where(c == 0, mine, other), jnp.where(c == 0, other, mine)
            both = jnp.concatenate([top, low], 0)
            moved = pltpu.roll(both, both.shape[0] - (top.shape[0] - OWN), 0)
            row = lax.broadcasted_iota(jnp.int32, both.shape, 0)
            merged[n, :, cols] = jnp.where(row < OWN, both, moved)[:PAIR].astype(bf16)

    def put(ref, n, first, size, i):
        copy = pltpu.make_async_copy(merged.at[n, :, pl.ds(first, size)], ref.at[c, block(me, PAIR)], ls.at[2 + i, n])
        copy.start()
        return copy

    halves = [Gather(pos, qkv0, (i * HD, HD), sems.at[i]) for i in range(LINES)]
    later = [Gather(pos, gu0, (F // LINES * i, F // LINES), sems.at[LINES + i]) for i in range(CORES)]
    across[0].wait()
    merge(0, 0, WIDE)
    put(qkv0, 0, 0, WIDE, 0).wait()
    for part in halves:
        part.start("z")
    merge(0, WIDE, WIDE + F)
    there = put(gu0, 0, WIDE, F, 1)
    across[1].wait()
    merge(1, 0, WIDE + F)
    rest = [there, put(qkv1, 1, 0, WIDE, 0), put(gu1, 1, WIDE, F, 1)]
    there.wait()
    for part in later:
        part.start("z")
    for part in halves:
        part.wait("z")
        part.start("ab", "near")
    fine, big = fine_ref[:], coarse_ref[:]
    n = fine.shape[1]
    for i in range(T // n):
        rows = slice(i * n, i * n + n)
        ca, sa = big[0, i : i + 1], big[1, i : i + 1]
        cos_ref[rows] = ca * fine[0] - sa * fine[1]
        sin_ref[rows] = sa * fine[0] + ca * fine[1]
    for part in halves:
        part.wait("ab")
        part.start("far", "mid")
    for part in halves:
        part.wait("far")
        part.start("last")
    for copy in local + rest[1:]:
        copy.wait()
    for part in halves:
        part.wait("near", "mid", "last")
    for part in later:
        part.wait("z")


def prologue(pack, wo, wd, coarse, fine):
    rows = pack.shape[2]
    full = [shape(CORES, D, WIDE)] * 2 + [shape(CORES, D, F)] * 2 + [shape(CHIPS, 2, wo.shape[1], D)] * 2 + [shape(CHIPS, 2, wd.shape[1], D)] * 2
    table = [shape(T, HALF, dtype=f32)] * 2
    whole = lambda a: const(*a.shape)
    got = pl.pallas_call(
        prologue_body, grid=(1,), in_specs=[whole(a) for a in (pack, wo, wd, coarse, fine)],
        out_specs=[whole(a) for a in table] + [HBM] * len(full), out_shape=table + full,
        scratch_shapes=[pltpu.VMEM((CORES, rows, pack.shape[3]), bf16), pltpu.VMEM((CORES, PAIR, pack.shape[3]), bf16), pltpu.SemaphoreType.DMA((CORES, 2)),
                        pltpu.SemaphoreType.DMA((LINES, 2)), pltpu.SemaphoreType.DMA((6, 2, GATHER_SEMS))],
        compiler_params=pltpu.CompilerParams(vmem_limit_bytes=LIMIT, collective_id=0, has_side_effects=True),
    )(pack, wo, wd, coarse, fine)
    return got[0], got[1], dict(zip(("qkv0", "qkv1", "gu0", "gu1", "wo0", "wo1", "wd0", "wd1"), got[2:]))


def turn(t, cos, sin):
    x, y = t[:, :HALF].astype(f32), t[:, HALF:].astype(f32)
    return jnp.concatenate([x * cos - y * sin, y * cos + x * sin], -1).astype(bf16)


def project_body(h_ref, w_ref, cos_ref, sin_ref, q_ref, k_ref, v_ref):
    a = normed(h_ref[:])
    cos, sin = cos_ref[:], sin_ref[:]
    for n, (owner, at, ref, head) in enumerate(((0, 0, q_ref, 0), (0, TILE, q_ref, 2), (1, 0, k_ref, 0), (1, TILE, v_ref, 0))):
        r = dot(a, w_ref[owner, :, at : at + TILE]).astype(bf16)
        for i in range(CORES):
            t = r[:, i * HD : i * HD + HD]
            ref[head + i] = turn(t, cos, sin) if ref is not v_ref else t


def project(h, w, cos, sin, *ride):
    rows = lambda width: along(0, TILE, width)
    heads = (HEADS, CORES, CORES)
    return call(project_body, (T // TILE,), (h, w, cos, sin), [rows(D), const(*w.shape), rows(HALF), rows(HALF)],
                [along(1, n, TILE, HD) for n in heads], [shape(n, T, HD) for n in heads], [], T * D * T * 2, *ride)


HIDDEN = -2e30
SCALE = HD**-0.5
EXP = SCALE * 1.4426950408889634
PIECES = [(i, n) for i in range(CORES) for n in range(CORES)]


def attend_body(q_ref, k_ref, v_ref, o_ref, lse_ref, top_s, mix_s):
    iq = pl.program_id(0)
    top_s[:] = jnp.full(top_s.shape, HIDDEN / 2, f32)
    mix_s[:] = jnp.zeros(mix_s.shape, f32)
    ones = jnp.ones((8, TILE), bf16)

    def keys(j, masked):
        here = block(j, TILE)
        scores = [dot_t(k_ref[i, here, :], q_ref[2 * i + n]) for i, n in PIECES]
        weights, keeps = [], []
        for m, s in enumerate(scores):
            if masked:
                s = jnp.where(lax.broadcasted_iota(jnp.int32, s.shape, 1) >= lax.broadcasted_iota(jnp.int32, s.shape, 0), s, HIDDEN)
            old = top_s[m : m + 1, :]
            top = jnp.maximum(old, s.max(axis=0, keepdims=True))
            top_s[m : m + 1, :] = top
            weights.append(jnp.exp2((s - top) * EXP).astype(bf16))
            keeps.append(jnp.exp2((old - top) * EXP))
        for m, (i, _) in enumerate(PIECES):
            values = jnp.concatenate([v_ref[i, here, :].T, ones], axis=0)
            mix_s[m] = mix_s[m] * keeps[m] + dot(values, weights[m])

    lax.fori_loop(0, iq, lambda j, _: keys(j, False), None)
    keys(iq, True)
    for m in range(len(PIECES)):
        total = mix_s[m, HD : HD + 1, :]
        o_ref[m] = (mix_s[m, :HD, :] * (1 / total)).T.astype(bf16)
        lse_ref[m] = top_s[m : m + 1, :] * SCALE + jnp.log(total)


def attend(q, k, v, *ride):
    tile = along(1, HEADS, TILE, HD)
    return call(attend_body, (T // TILE,), (q, k, v), [tile, const(*k.shape), const(*v.shape)],
                [tile, along(2, HEADS, 1, TILE)], [shape(HEADS, T, HD), shape(HEADS, 1, T, dtype=f32)],
                [pltpu.VMEM((HEADS, TILE), f32), pltpu.VMEM((HEADS, HD + 8, TILE), f32)], 4 * 2 * T * T * HD, *ride)


def gate_up_body(o_ref, wo_ref, h_ref, wg_ref, wu_ref, h2_ref, g_ref, u_ref, p_ref, b_s):
    j, t = pl.program_id(0), pl.program_id(1)
    tm = g_ref.shape[0]

    @pl.when(j == 0)
    def _():
        rows = block(t, tm)
        acc = sum(dot(o_ref[n, rows, :], wo_ref[4 * n : 4 * n + 4].reshape(HD, D)) for n in range(LINES))
        h2 = h_ref[rows] + acc.astype(bf16)
        h2_ref[rows] = h2
        b_s[rows] = normed(h2)

    sub = 256
    for m in range(tm // sub):
        here = cut(m, sub)
        b = b_s[block(t * (tm // sub) + m, sub), :]
        g, u = dot(b, wg_ref[0]), dot(b, wu_ref[0])
        g_ref[here] = g
        u_ref[here] = u
        p_ref[here] = (g * jax.nn.sigmoid(g) * u).astype(bf16)


def gate_up(o, wo, h, gu, *ride):
    tm = 1024
    tile = pl.BlockSpec((tm, TILE), lambda j, t: (t, j))
    weight = lambda i: pl.BlockSpec((1, D, TILE), lambda j, t: (i, 0, j))
    return call(gate_up_body, (F // TILE, T // tm), (o, wo, h, gu, gu), [const(*o.shape), const(*wo.shape), const(*h.shape), weight(0), weight(1)],
                [const(T, D), tile, tile, tile], [shape(T, D), shape(T, F, dtype=f32), shape(T, F, dtype=f32), shape(T, F)],
                [pltpu.VMEM((T, D), bf16)], 2 * T * D * (D + 2 * F), *ride)


def down_body(p_ref, wd_ref, h2_ref, h3_ref):
    acc = dot(p_ref[:], wd_ref[:])
    h3_ref[:] = h2_ref[:] + acc.astype(bf16)


def down(p, wd, h2, *ride):
    rows = lambda n: along(0, TILE, n)
    return call(down_body, (T // TILE,), (p, wd.reshape(F, D), h2), [rows(F), const(F, D), rows(D)], [rows(D)], [shape(T, D)], [], 2 * T * D * F, *ride)


PLANS = (
    dict(
        project=("gu0[0:2],ab.0.1,far.1.3,last.3.e", "gu0[2:4],ab.0.2,far.2.e,last.e.e", "gu0[4:8],z.0.e", "wo0,z.0.e"),
        attend=("wo0,ab.0.1,far.1.2,last.2.e", "gu0[4:8],ab.0.2,far.2.e,last.e.e", "wd0,z.0.e"),
        gate_up=("wd0,ab.0.5,far.5.9,last.9.e", "qkv1,z.0.5,ab.5.e", "gu1[0:2],z.5.9,ab.9.e", "gu1[2:4],z.5.e"),
        down=("qkv1,far.0.2,last.2.e", "gu1[0:2],far.0.e", "gu1[2:4],ab.0.e", "gu1[4:6],z.0.e"),
    ),
    dict(
        project=("gu1[0:2],last.0.e", "gu1[2:4],far.0.e", "gu1[4:6],ab.0.e", "gu1[6:8],z.0.e", "wo1,z.0.e"),
        attend=("gu1[2:4],last.0.e", "gu1[4:6],far.0.3,last.3.e", "gu1[6:8],ab.0.3,far.3.e,last.e.e", "wo1,ab.0.3,far.3.e,last.e.e", "wd1,z.0.e"),
        gate_up=("wd1,ab.0.6,far.6.10,last.10.e",),
    ),
)


def read_plan(text):
    name, *todo = text.split(",")
    name, _, cols = name.rstrip("]").partition("[")
    if cols:
        first, end = (F // 8 * int(n) for n in cols.split(":"))
        cols = (first, end - first)
    phases = [item.split(".") for item in todo]
    return name, cols, {phase: [END if k == "e" else int(k) for k in steps] for phase, *steps in phases}


def forward(x, pack, wo, wd, coarse, fine):
    cos, sin, arrays = prologue(pack, wo, wd, coarse, fine)
    h, kept, cid = x, [], 1
    for n, texts in enumerate(PLANS):
        plan = {name: [read_plan(item) for item in text] for name, text in texts.items()}
        q, k, v = project(h, arrays[f"qkv{n}"], cos, sin, arrays, plan["project"], cid)
        o, lse = attend(q, k, v, arrays, plan["attend"], cid + 1)
        h2, g, u, p = gate_up(o, arrays[f"wo{n}"], h, arrays[f"gu{n}"], arrays, plan["gate_up"], cid + 2)
        kept.append((h, q, k, v, o, lse, h2, g, u, p))
        if n == 0:
            h, = down(p, arrays["wd0"], h2, arrays, plan["down"], cid + 3)
        cid += 4
    return cos, sin, arrays, kept


def ring_scratch(rows, width, slots, late=0):
    line = LINES * rows
    dims = ((slots, CORES, LINES * line), (slots, LINES * line), (slots, CORES, line), (slots, line), (late or slots, LINES, rows), (slots, LINES - 1, rows))
    return [pltpu.VMEM((*d, width), bf16) for d in dims] + [pltpu.SemaphoreType.DMA((slots, 2, 7))]


RING = 7


class Ring:
    def __init__(self, pos, refs):
        self.pos = pos
        self.my, self.rd, self.rb, self.ra, self.zs, self.rz, self.sems = refs
        self.rows = self.zs.shape[2]
        self.late = lambda slot: jnp.minimum(slot, self.zs.shape[0] - 1)

    def line(self, l):
        return block(l, LINES * self.rows)

    def copies(self, slot, stage, source=None):
        p, peer, sems = self.pos, self.pos["peer"], self.sems.at[slot]
        mine = self.my.at[slot, p["c"]]
        if stage == 0:
            source = self.my.at[slot] if source is None else source
            return [remote(source.at[1 - p["c"]], self.rd.at[slot], sems, 0, peer["d"])]
        if stage == 1:
            return [remote(mine.at[self.line(p[name])], self.rb.at[slot, i], sems, 1 + i, peer["b"]) for i, name in enumerate(("lb", "ld"))]
        if stage == 2:
            return [remote(mine.at[self.line(p["la"])], self.ra.at[slot], sems, 3, peer["a"])]
        return [remote(self.zs.at[self.late(slot), lax.rem(p["z"] + k, LINES)], self.rz.at[slot, k - 1], sems, 3 + k, peer[k]) for k in range(1, LINES)]

    def send(self, slot, stage=0, source=None):
        for copy in self.copies(slot, stage, source):
            copy.start()

    def add(self, slot, l, theirs):
        n, size = LINES * self.rows, 32
        c = self.pos["c"]

        def some(i, _):
            here, there = pl.ds(pl.multiple_of(n * l + i * size, size), size), pl.ds(pl.multiple_of(i * size, size), size)
            self.my[slot, c, here, :] = (self.my[slot, c, here, :].astype(f32) + theirs[there, :].astype(f32)).astype(bf16)

        lax.fori_loop(0, n // size, some, None)

    def stage(self, slot, n):
        p = self.pos
        for copy in self.copies(slot, n - 1):
            copy.wait()
        if n == 1:
            for l in range(LINES):
                self.add(slot, l, self.rd.at[slot, self.line(l)])
        elif n == 2:
            self.add(slot, p["own"], self.rb.at[slot, 0])
            self.add(slot, p["la"], self.rb.at[slot, 1])
        elif n == 3:
            mine = self.my[slot, p["c"], self.line(p["own"]), :].astype(f32)
            self.zs[self.late(slot)] = (mine + self.ra[slot].astype(f32)).reshape(LINES, self.rows, -1).astype(bf16)
        else:
            return (self.zs[self.late(slot), p["z"]].astype(f32) + sum(self.rz[slot, k].astype(f32) for k in range(LINES - 1))).astype(bf16)
        self.send(slot, n)


def drain(units):
    while units:
        for ring, slot, n, end in units:
            ring.stage(slot, n) if n < 4 else end()
        units = [(ring, slot, n + 1, end) for ring, slot, n, end in units if n < 4]


def finish(copies):
    for copy in copies:
        copy.wait()


def ffn_back_body(h2_ref, dy_ref, p_ref, g_ref, u_ref, wg_ref, wu_ref, wd_ref, o_ref, wo_ref, fin, late_out, wd_out, dh_ref, do_ref, dwo_ref,
                  b_s, db_s, dg_s, du_s, ls, *rest):
    j, t = pl.program_id(0), pl.program_id(1)
    tm, nj, nt = g_ref.shape[0], pl.num_programs(0) - 1, pl.num_programs(1) - 1
    pos = place()
    gu, wd = Ring(pos, rest[:RING]), Ring(pos, rest[RING:])
    slot, old = lax.rem(j, 2), lax.rem(j + 1, 2)
    third = lambda n: lax.rem(n, 3)
    newest, oldest = third(j + 2), third(j + 1)
    at = lambda k, *also: functools.partial(pl.when, functools.reduce(lambda a, b: a & b, also, t == k))()
    at(0, j == 0)(lambda: greet(pos))
    sub = 256
    n_last = F // TILE - 1
    more, both, ours, late = j >= 1, j >= 2, (j >= 1) & (j < nj), j == nj - 1

    def gu_end():
        fin[:, block(j - 2, TILE)] = gu.stage(slot, 4)

    def wd_end(j):
        wd_out[:, block(j, HALF)] = wd.stage(third(j), 4)

    at(0, both)(lambda: wd.stage(oldest, 3))
    at(0, more)(lambda: wd.stage(newest, 1))
    at(1, both)(lambda: gu.stage(slot, 3))
    at(1, ours)(lambda: gu.stage(old, 1))
    at(2, j == nj)(lambda: wd.stage(newest, 2))

    @at(3, j == nj)
    def _():
        wd_end(j - 2)
        wd.stage(newest, 3)


    @at(4, ours)
    def _():
        gu.stage(old, 2)
        wd.stage(newest, 2)


    at(4, both)(gu_end)
    at(4, both & ours)(lambda: wd_end(j - 2))

    @pl.when((t < nt) & (j < nj))
    def _():
        rows = block(t, tm)

        @pl.when(j == 0)
        def _():
            b_s[rows] = normed(h2_ref[rows])
            db_s[rows] = jnp.zeros((tm, D), f32)

        for m in range(tm // sub):
            here, rows = cut(m, sub), block(t * (tm // sub) + m, sub)
            dp = dot_t(dy_ref[rows], wd_ref[:]).astype(bf16).astype(f32)
            g, u = g_ref[here], u_ref[here]
            s = jax.nn.sigmoid(g)
            gs = g * s
            du = (dp * gs).astype(bf16)
            dg = (dp * u * (s + gs * (1 - s))).astype(bf16)
            dg_s[rows] = dg
            du_s[rows] = du
            db_s[rows] += dot_t(dg, wg_ref[0]) + dot_t(du, wu_ref[0])

        @pl.when(late)
        def _():
            for m in range(tm // sub):
                rows = block(t * (tm // sub) + m, sub)
                dh_ref[rows] = norm_back(h2_ref[rows].astype(f32), db_s[rows], dy_ref[rows])

    rows = wd.rows
    for n in range(LINES):

        @pl.when((t > 0) & (j == 2 * n))
        def _():
            r = t_dot(p_ref[:], dy_ref[:, sub * n : min(sub * n + sub, D)]).astype(bf16)
            for q in range(D // rows):
                at = pl.multiple_of(LINES * rows * (t - 1) + rows * (q // CORES), rows)
                for e in range(r.shape[1] // HALF):
                    wd.my[(2 * n + e) % 3, q % CORES, pl.ds(at, rows), :] = r[cut(q, rows), cut(e, HALF)]

    at(4, j < nj)(lambda: wd.send(third(j)))

    @at(4, j < nj)
    def _():
        for i, ref in enumerate((dg_s, du_s)):
            for n in range(TILE // sub):
                cols = cut(n, sub)
                gu.my[slot, i, :, cols] = t_dot(b_s[:], ref[:, cols]).astype(bf16)
        pl.when(j < nj - 1)(lambda: gu.send(slot))

    save = pltpu.make_async_copy(gu.my.at[n_last % 2], late_out, ls)
    at(4, late)(lambda: save.start())

    @pl.when((j == nj) & (t < nt))
    def _():
        do_ref[0] = dot_t(dh_ref[:], wo_ref[:].reshape(HD, D)).astype(bf16)
        r = t_dot(o_ref[0], dh_ref[:]).astype(bf16).reshape(*wo_ref.shape)
        for i in range(CORES):
            dwo_ref[i] = r[:, i].reshape(HALF, D)

    @at(4, j == nj)
    def _():
        wd_end(n_last)
        save.wait()


def ffn_back(h2, dy, p, g, u, gu, wd, o, wo, cid):
    tm = 512
    nj, nt = F // TILE, T // tm
    tj = lambda j: jnp.minimum(j, nj - 1)
    tt = lambda j, t: jnp.where(j < nj, jnp.minimum(t, nt - 1), nt - 1)
    head = lambda j, t: jnp.where(j < nj, 0, jnp.minimum(t, nt - 1))
    weight = lambda i: pl.BlockSpec((1, D, TILE), lambda j, t: (i, 0, tj(j)))
    tile = pl.BlockSpec((tm, TILE), lambda j, t: (tt(j, t), tj(j)))
    one = pl.BlockSpec((1, T, HD), lambda j, t: (head(j, t), 0, 0))
    rows, done = F // CHIPS // CORES, F - TILE
    return pl.pallas_call(
        ffn_back_body, grid=(nj + 1, nt + 1),
        in_specs=[const(T, D), const(T, D), pl.BlockSpec((T, D), lambda j, t: (0, jnp.where(lax.rem(j, 2) > 0, nt - 1, jnp.maximum(t - 1, 0)))), tile, tile,
                  weight(0), weight(1), pl.BlockSpec((TILE, D), lambda j, t: (tj(j), 0)), one,
                  pl.BlockSpec((4, *wo.shape[1:]), lambda j, t: (head(j, t), 0, 0, 0))],
        out_specs=[const(PAIR, done), HBM, const(rows, D), const(T, D), one, pl.BlockSpec((CORES, HALF, D), lambda j, t: (0, head(j, t), 0))],
        out_shape=[shape(PAIR, done), shape(CORES, D, TILE), shape(rows, D), shape(T, D), shape(HEADS, T, HD), shape(CORES, TILE, D)],
        scratch_shapes=[pltpu.VMEM((T, D), bf16), pltpu.VMEM((T, D), f32), pltpu.VMEM((T, TILE), bf16), pltpu.VMEM((T, TILE), bf16)]
        + [pltpu.SemaphoreType.DMA(())] + ring_scratch(PAIR, TILE, 2, 1) + ring_scratch(rows, HALF, 3, 1),
        compiler_params=pltpu.CompilerParams(vmem_limit_bytes=LIMIT, collective_id=cid, has_side_effects=True),
        cost_estimate=pl.CostEstimate(flops=12 * T * D * F, bytes_accessed=F * T * 12, transcendentals=0),
    )(h2, dy, p, g, u, gu, gu, wd.reshape(F, D), o, wo)


DUE = ((4, 6), (6, 8), (7, 8), (8,))


def attend_back_body(q_ref, k_ref, v_ref, do_ref, o_ref, lse_ref, wo_in, *refs, units):
    given, refs = refs[:units], refs[units:]
    dq_ref, dk_ref, dv_ref, wo_out, fin, dq_s, dk_s, dv_s, delta_s, loads, *rest = refs
    iq = pl.program_id(0)
    pos = place()
    wide, wo = Ring(pos, rest[:RING]), Ring(pos, rest[RING:])
    todo = [(wide, 0, given[0]), (wo, 0, wo_in)] + [(wide, 1 + i, ref.at[i]) for ref in given[1:] for i in range(CORES)]
    mine = [pltpu.make_async_copy(ref.at[pos["c"]], ring.my.at[slot, pos["c"]], loads.at[i]) for i, (ring, slot, ref) in enumerate(todo)]

    def end(ring, slot):
        if ring is wo:
            wo_out[:] = ring.stage(slot, 4)
        else:
            fin[:, TILE * slot : TILE * slot + TILE] = ring.stage(slot, 4)

    def event(e):
        @pl.when(e == 1)
        def _():
            for copy, (ring, slot, _) in zip(mine, todo):
                copy.wait()
                ring.stage(slot, 1)

        for (ring, slot, _), steps in zip(todo, DUE):
            for n, k in enumerate(steps):
                pl.when(e == k)(functools.partial(ring.stage, slot, n + 2))

    @pl.when(iq == 0)
    def _():
        for copy in mine:
            copy.start()
        greet(pos)
        for ring, slot, ref in todo:
            ring.send(slot, 0, ref)
        dk_s[:] = jnp.zeros_like(dk_s)
        dv_s[:] = jnp.zeros_like(dv_s)

    dq_s[:] = jnp.zeros_like(dq_s)
    for m in range(len(PIECES)):
        x = do_ref[m].astype(f32) * o_ref[m].astype(f32)
        delta_s[m] = (x[:, :HALF] + x[:, HALF:]).T.sum(axis=0, keepdims=True)

    def keys(j, masked):
        here = block(j, TILE)
        scores = [dot_t(k_ref[i, here, :], q_ref[2 * i + n]) for i, n in PIECES]
        dps = [dot_t(v_ref[i, here, :], do_ref[2 * i + n]) for i, n in PIECES]
        for m, (i, n) in enumerate(PIECES):
            p = jnp.exp2(scores[m] * EXP - lse_ref[m] * (EXP / SCALE))
            if masked:
                p = jnp.where(lax.broadcasted_iota(jnp.int32, p.shape, 1) >= lax.broadcasted_iota(jnp.int32, p.shape, 0), p, 0.0)
            ds = (p * (dps[m] - delta_s[m])).astype(bf16)
            dv_s[i, here, :] += dot(p.astype(bf16), do_ref[m])
            dk_s[i, here, :] += dot(ds, q_ref[m])
            dq_s[m] += dot(k_ref[i, here, :].T, ds)

    @functools.partial(lax.fori_loop, 0, iq, init_val=None)
    def _(j, _):
        event(lax.div(iq * (iq + 1), 2) + j)
        keys(j, False)

    keys(iq, True)
    for m in range(len(PIECES)):
        dq_ref[m] = (dq_s[m] * SCALE).T.astype(bf16)

    @pl.when(iq == pl.num_programs(0) - 1)
    def _():
        dk_ref[:] = (dk_s[:] * SCALE).astype(bf16)
        dv_ref[:] = dv_s[:].astype(bf16)
        drain([(ring, slot, 2 + len(steps), functools.partial(end, ring, slot)) for (ring, slot, _), steps in zip(todo, DUE)])


def attend_back(q, k, v, do, o, lse, dwo, units, cid):
    tile = along(1, HEADS, TILE, HD)
    keys, rows, n = const(*k.shape), D // OWN, len(units)
    n_wide = CORES * n - 1
    return pl.pallas_call(
        functools.partial(attend_back_body, units=n), grid=(T // TILE,),
        in_specs=[tile, keys, keys, tile, tile, along(2, HEADS, 1, TILE)] + [HBM] * (1 + n),
        out_specs=[tile, keys, keys, const(rows, D), const(PAIR, n_wide * TILE)],
        out_shape=[shape(*a.shape) for a in (q, k, v)] + [shape(rows, D), shape(PAIR, n_wide * TILE)],
        scratch_shapes=[pltpu.VMEM((HEADS, HD, TILE), f32), pltpu.VMEM(k.shape, f32), pltpu.VMEM(k.shape, f32), pltpu.VMEM((HEADS, 1, TILE), f32)]
        + [pltpu.SemaphoreType.DMA((1 + n_wide,))] + ring_scratch(PAIR, TILE, n_wide) + ring_scratch(rows, D, 1),
        compiler_params=pltpu.CompilerParams(vmem_limit_bytes=LIMIT, collective_id=cid, has_side_effects=True),
        cost_estimate=pl.CostEstimate(flops=20 * T * T * HD, bytes_accessed=T * D * 12, transcendentals=0),
    )(q, k, v, do, o, lse, dwo, *units)


def turn_back(ref, g_s, first, *angles):
    sub = 512
    for i in range(ref.shape[0]):
        at = first + i * HD
        for m in range(0, T, sub):
            rows = slice(m, m + sub)
            t = ref[i, rows, :]
            g_s[rows, at : at + HD] = turn(t, angles[0][rows], -angles[1][rows]) if angles else t


def qkv_back_body(dq_ref, dk_ref, dv_ref, cos_ref, sin_ref, h_ref, w_ref, dh2_ref, dw_ref, dh_ref, a_s, g_s, da_s):
    s = pl.program_id(0)
    sub = 512
    pieces = [slice(m, m + sub) for m in range(0, T, sub)]

    @pl.when(s == 0)
    def _():
        for m in pieces:
            a_s[m] = normed(h_ref[m])
            da_s[m] = jnp.zeros((sub, D), f32)

    for k, ref in enumerate((dq_ref, dk_ref, dq_ref, dv_ref)):
        angles = () if ref is dv_ref else (cos_ref, sin_ref)
        pl.when(s == k)(functools.partial(turn_back, ref, g_s, 0, *angles))
    dw_ref[0, 0] = t_dot(a_s[:], g_s[:]).astype(bf16)
    for m in pieces:
        da_s[m] += dot_t(g_s[m], w_ref[0])

    @pl.when(s == 3)
    def _():
        for m in pieces:
            dh_ref[m] = norm_back(h_ref[m].astype(f32), da_s[m], dh2_ref[m])


def qkv_back(dq, dk, dv, cos, sin, h, w, dh2):
    keys = const(*dk.shape)
    return call(qkv_back_body, (HEADS,), (dq, dk, dv, cos, sin, h, w, dh2),
                [pl.BlockSpec((CORES, T, HD), lambda s: (lax.div(s, 2), 0, 0)), keys, keys, const(T, HALF), const(T, HALF), const(T, D),
                 pl.BlockSpec((1, D, TILE), lambda s: (lax.rem(s, 2), 0, lax.div(s, 2))), const(T, D)],
                [pl.BlockSpec((1, 1, D, TILE), lambda s: (lax.div(s, 2), lax.rem(s, 2), 0, 0)), const(T, D)], [shape(CORES, 2, D, TILE), shape(T, D)],
                [pltpu.VMEM((T, D), bf16), pltpu.VMEM((T, TILE), bf16), pltpu.VMEM((T, D), f32)], 4 * T * D * 4 * TILE)


def qkv_last_body(dq_ref, dk_ref, dv_ref, cos_ref, sin_ref, h_ref, fin, a_s, g_s, *rest):
    pos = place()
    ring = Ring(pos, rest)
    s = pl.program_id(0)

    @pl.when(s == 0)
    def _():
        greet(pos)
        a_s[:] = normed(h_ref[:])

    turn_back(dq_ref, g_s, 0, cos_ref, sin_ref)
    pl.when(s < 2)(lambda: turn_back(dk_ref, g_s, HD, cos_ref, sin_ref))
    pl.when(s >= 2)(lambda: turn_back(dv_ref, g_s, HD))
    for i in range(CORES):
        ring.my[s, i] = t_dot(a_s[:], g_s[:, HD * i : HD * i + HD]).astype(bf16)
    ring.send(s)

    def end(slot):
        fin[:, HD * slot : HD * slot + HD] = ring.stage(slot, 4)

    for k in range(1, 4):
        for n in range(1, k + 1):
            pl.when(s == k)(functools.partial(ring.stage, k - n, n))

    @pl.when(s == 3)
    def _():
        drain([(ring, slot, 4 - slot, functools.partial(end, slot)) for slot in range(LINES)])


def qkv_last(dq, dk, dv, cos, sin, h, cid):
    head = lambda n, of: pl.BlockSpec((1, T, HD), lambda s: (jnp.clip(s - n, 0, of - 1), 0, 0))
    return pl.pallas_call(
        qkv_last_body, grid=(HEADS,), in_specs=[head(0, 4), head(0, 2), head(2, 2), const(T, HALF), const(T, HALF), const(T, D)], out_specs=const(PAIR, WIDE),
        out_shape=shape(PAIR, WIDE),
        scratch_shapes=[pltpu.VMEM((T, D), bf16), pltpu.VMEM((T, TILE), bf16)] + ring_scratch(PAIR, HD, 4),
        compiler_params=pltpu.CompilerParams(vmem_limit_bytes=LIMIT, collective_id=cid, has_side_effects=True),
        cost_estimate=pl.CostEstimate(flops=2 * T * D * 4 * TILE, bytes_accessed=T * D * 10, transcendentals=0),
    )(dq, dk, dv, cos, sin, h)


def sources(gu, late, qkv, first):
    wide = F - TILE
    pair = lambda owner: [(gu, owner, 0, 0, wide), (late, owner, 0, wide, TILE)]
    return [[(qkv, 0, first, 0, WIDE)], [(qkv, 1, first, 0, TILE)], [(qkv, 1, first + TILE, 0, TILE)], pair(0), pair(1)]


def own_rows(c, both, owner, cols):
    mine, theirs = (ref[:, cols].astype(f32) for ref in both)
    x = jnp.where(c == owner, mine, theirs)
    return jnp.where(c == 0, x, pltpu.roll(x, OWN, 0))[:OWN]


def lay_out(c, pairs, outs):
    gu0, late0, last0, gu1, late1 = pairs
    for n, from_layer in enumerate((sources(gu0, late0, last0, 0), sources(gu1, late1, late0, TILE))):
        for out, parts in zip(outs, from_layer):
            for ref, owner, at, to, width in parts:
                for k in range(0, width, TILE):
                    out[:, n, to + k : to + k + TILE] = own_rows(c, ref, owner, slice(at + k, at + k + TILE))


def squares_body(*refs, n_sums, n_halved):
    sums, out_ref, grads = refs[:n_sums], refs[n_sums], refs[n_sums + 1 : -4 - n_halved]
    *others, mine, parts, swap, sems = refs[-4 - n_halved :]
    pos = place()
    greet(pos)
    halved = sums[:n_halved]
    across = [remote(ref, other, swap, i, pos["peer"]["d"]) for i, (ref, other) in enumerate(zip(halved, others))]
    for copy in across:
        copy.start()
    total = jnp.zeros((1, HALF), f32)
    for ref in sums:
        for at in range(0, ref.shape[1], HALF):
            x = ref[:, at : at + HALF].astype(f32)
            total += (x * x).sum(axis=0, keepdims=True)
    mine[:] = jnp.broadcast_to(total, mine.shape)
    n = 0
    for names in ("d", "a", "b", range(1, LINES)):
        copies = [remote(mine, parts.at[n + i], sems, n + i, pos["peer"][name]) for i, name in enumerate(names)]
        for copy in copies:
            copy.start()
        if n == 1:
            finish(across)
            lay_out(pos["c"], list(zip(halved, others)), grads)
        finish(copies)
        mine[:] += sum(parts[n + i] for i in range(len(names)))
        n += len(names)
    out_ref[:] = mine[:]


def squares(halved, whole, cid):
    part, peers, sums = (8, HALF), LINES + 2, (*halved, *whole)
    outs = [shape(*part, dtype=f32)] + [shape(OWN, 2, n, dtype=f32) for n in (WIDE, TILE, TILE, F, F)]
    return pl.pallas_call(
        functools.partial(squares_body, n_sums=len(sums), n_halved=len(halved)), grid=(1,), in_specs=[const(*a.shape) for a in sums],
        out_specs=[const(*a.shape) for a in outs], out_shape=outs,
        scratch_shapes=[pltpu.VMEM(a.shape, bf16) for a in halved]
        + [pltpu.VMEM(part, f32), pltpu.VMEM((peers, *part), f32), pltpu.SemaphoreType.DMA((CORES, len(halved))), pltpu.SemaphoreType.DMA((CORES, peers))],
        compiler_params=pltpu.CompilerParams(vmem_limit_bytes=LIMIT, collective_id=cid, has_side_effects=True),
    )(*sums)


def adamw(w, m, v, g):
    m = 0.9 * m + 0.1 * g
    v = 0.95 * v + 0.05 * g * g
    step = m * lax.rsqrt(v + 1e-8) + 0.1 * w
    return (w - 0.02 * step).astype(bf16), m, v


def update(halved, whole, weights, m, v, cid):
    total, *grads = squares(halved, whole, cid)
    count = 2 * CHIPS * sum(w.size for w in weights)
    factor = jnp.minimum(1.0, 0.5 * lax.rsqrt(total[0].sum() / count + 1e-30))
    q, k, vv, gate, up = (g.transpose(1, 0, 2) for g in grads)
    o0, d0, o1, d1 = whole
    both = lambda *layers: jnp.stack(layers).astype(f32)
    grads = q, k, vv, both(o0, o1), gate, up, both(d0, d1)
    new = [adamw(w.astype(f32), m, v, g * factor) for w, m, v, g in zip(weights, m, v, grads, strict=True)]
    return tuple(one[which] for which in range(3) for one in new)


def tables():
    freq, fine = THETA ** (-jnp.arange(HALF, dtype=f32) / HALF), 64
    angles = [jnp.arange(n, dtype=f32)[:, None] * step * freq for n, step in ((T // fine, fine), (fine, 1))]
    return [jnp.stack([jnp.cos(a), jnp.sin(a)]) for a in angles]


def solution(mesh):
    def step(x, dy, *arrays):
        wq, wk, wv, wo, wg, wu, wd = arrays[:7]
        pack = jnp.stack([jnp.pad(jnp.concatenate(parts, -1), ((0, 0), (0, 4), (0, 0))) for parts in ((wq, wg), (wk, wv, wu))])
        cos, sin, full, kept = forward(x[0], pack, wo, wd, *tables())
        by_h, late, halved, whole = dy[0], [], [], []
        for n in (1, 0):
            h, q, k, vv, o, lse, h2, g, u, p = kept[n]
            s_gu, last, s_d, dh2, do, dwo = ffn_back(h2, by_h, p, g, u, full[f"gu{n}"], full[f"wd{n}"], o, full[f"wo{n}"], 8)
            dq, dk, dv, s_o, s_late = attend_back(q, k, vv, do, o, lse, dwo, [last, *late], 9 + n)
            if n:
                dqkv, by_h = qkv_back(dq, dk, dv, cos, sin, h, full[f"qkv{n}"], dh2)
                late = [dqkv]
            last = [] if n else [qkv_last(dq, dk, dv, cos, sin, h, 11)]
            halved, whole = [s_gu, s_late, *last, *halved], [s_o, s_d, *whole]
        return update(halved, whole, *(arrays[i : i + 7] for i in (0, 7, 14)), 12)

    states, cut = P(("rep", "dp")), P(None, "dp")
    return jax.shard_map(step, mesh=mesh, in_specs=(states, states) + (cut,) * 21, out_specs=(P("rep", "dp"),) * 21, check_vma=False)
```

```python
import functools

import jax
import jax.numpy as jnp
from jax import lax
from jax.experimental import pallas as pl
from jax.experimental.pallas import tpu as pltpu
from jax.sharding import PartitionSpec as P

T, D, F, HD, TILE = 2048, 896, 3584, 256, 512
HALF, WIDE = HD // 2, 2 * TILE
CHIPS, LINES, CORES, HEADS = 16, 4, 2, 4
OWN = 28
PAIR = 2 * OWN
LIMIT = 67043328
f32, bf16 = jnp.float32, jnp.bfloat16
THETA = 10000
HBM = pl.BlockSpec(memory_space=pltpu.HBM)


def dot(a, b, ca=1, cb=0):
    return lax.dot_general(a, b, (((ca,), (cb,)), ((), ())), preferred_element_type=f32)


def dot_t(a, b):
    return dot(a, b, 1, 1)


def t_dot(a, b):
    return dot(a, b, 0, 0)


def rms(h):
    return lax.rsqrt(jnp.mean(h * h, -1, keepdims=True) + 1e-6)


def normed(h):
    h = h.astype(f32)
    return (h * rms(h)).astype(bf16)


def norm_back(h, db, dres):
    s = rms(h)
    m = jnp.mean(h * db, -1, keepdims=True)
    return dres + (s * db - h * (s * s * s * m)).astype(bf16)


def const(*shape):
    return pl.BlockSpec(shape, lambda *i: (0,) * len(shape), pipeline_mode=pl.Buffered(1))


def shape(*dims, dtype=bf16):
    return jax.ShapeDtypeStruct(dims, dtype)


def cut(i, n):
    return slice(i * n, i * n + n)


def along(axis, *block):
    return pl.BlockSpec(block, lambda i: tuple(i if k == axis else 0 for k in range(len(block))))


def block(at, n):
    return pl.ds(pl.multiple_of(at * n, n), n)


def place():
    me = lax.axis_index("dp")
    c, z, own = lax.rem(me, CORES), lax.rem(lax.div(me, CORES), LINES), lax.div(me, CORES * LINES)
    at = lambda line, z, c: (line * LINES + z) * CORES + c
    flip_x, flip_y = lax.rem(own + 2, LINES), own + 1 - 2 * lax.rem(own, 2)
    la, lb = jnp.where(c == 0, flip_y, flip_x), jnp.where(c == 0, flip_x, flip_y)
    peer = dict(d=at(own, z, 1 - c), a=at(la, z, c), b=at(lb, z, c))
    for k in range(1, LINES):
        peer[k] = at(own, lax.rem(z + k, LINES), c)
    return dict(c=c, z=z, own=own, la=la, lb=lb, ld=LINES - 1 - own, peer=peer)


def greet(pos):
    bar = pltpu.get_barrier_semaphore()
    for n in pos["peer"].values():
        pl.semaphore_signal(bar, inc=1, device_id=(0, n), device_id_type=pl.DeviceIdType.MESH)
    pl.semaphore_wait(bar, len(pos["peer"]))


def remote(src, dst, sems, i, device):
    return pltpu.make_async_remote_copy(src_ref=src, dst_ref=dst, send_sem=sems.at[0, i], recv_sem=sems.at[1, i], device_id=(0, device),
                                        device_id_type=pl.DeviceIdType.MESH)


class Gather:
    def __init__(self, pos, ref, cols, sems):
        self.pos, self.ref, self.cols, self.sems = pos, ref, cols, sems

    def part(self, chip, n):
        c = self.pos["c"]
        if len(self.ref.shape) > 3:
            return self.ref.at[pl.ds(chip, n), c]
        rows = block(chip if n == 1 else lax.div(chip, n), n * PAIR)
        return self.ref.at[c, rows, pl.ds(*self.cols)] if self.cols else self.ref.at[c, rows]

    def copies(self, what):
        p = self.pos
        peer, line = p["peer"], lambda name: self.part(LINES * p[name], LINES)
        mine = self.part(LINES * p["own"] + p["z"], 1)
        todo = dict(z=[(mine, k) for k in range(1, LINES)], ab=[(line("own"), "a"), (line("own"), "b")], far=[(line("la"), "b")],
                    near=[(line("own"), "d")], mid=[(line("la"), "d"), (line("lb"), "d")], last=[(line("ld"), "d")])
        first = 0
        for name, items in todo.items():
            if name == what:
                return [remote(src, src, self.sems, first + i, peer[to]) for i, (src, to) in enumerate(items)]
            first += len(items)

    def start(self, *names):
        for name in names:
            for copy in self.copies(name):
                copy.start()

    def wait(self, *names):
        for name in names:
            for copy in self.copies(name):
                copy.wait()


GATHER_SEMS = 10


PHASES = dict(z=("z",), ab=("ab", "near"), far=("far", "mid"), last=("last",))
END = 99


class Ride:
    def __init__(self, refs, plan, sems, step, last):
        self.pos, self.step, self.last = place(), step, last
        self.items = [(Gather(self.pos, refs[name], cols, sems.at[i]), phases) for i, (name, cols, phases) in enumerate(plan)]

    def do(self, phase, i, k):
        for part, phases in self.items:
            if phase in phases and phases[phase][i] == k:
                (part.wait if i else part.start)(*PHASES[phase])

    def run(self, k):
        if k < END:
            for phase in PHASES:
                self.do(phase, 1, k)
            for phase in reversed(PHASES):
                self.do(phase, 0, k)
        else:
            for phase in PHASES:
                self.do(phase, 0, k)
                self.do(phase, 1, k)

    def before(self):
        pl.when(self.step == 0)(lambda: greet(self.pos))
        for k in sorted({k for _, phases in self.items for pair in phases.values() for k in pair} - {END}):
            pl.when(self.step == k)(functools.partial(self.run, k))

    def after(self):
        pl.when(self.step == self.last)(functools.partial(self.run, END))


def call(body, grid, ins, in_specs, out_specs, outs, scratch, flops, arrays=(), plan=(), cid=None):
    names = sorted({item[0] for item in plan})
    n_in, n_out, n_scratch, n = len(ins), len(outs), len(scratch), len(names)

    def kernel(*refs):
        given, refs = refs[:n_in], refs[n_in + n :]
        made, carried, refs = refs[:n_out], refs[n_out : n_out + n], refs[n_out + n :]
        step = pl.program_id(0)
        last = grid[0] - 1
        for i, size in enumerate(grid[1:]):
            step, last = step * size + pl.program_id(i + 1), (last + 1) * size - 1
        if not plan:
            return body(*given, *made, *refs)
        ride = Ride(dict(zip(names, carried)), plan, refs[n_scratch], step, last)
        ride.before()
        body(*given, *made, *refs[:n_scratch])
        ride.after()

    extra = [arrays[name] for name in names]
    got = pl.pallas_call(
        kernel, grid=grid, in_specs=list(in_specs) + [HBM] * n, out_specs=list(out_specs) + [HBM] * n,
        out_shape=list(outs) + [shape(*a.shape) for a in extra],
        scratch_shapes=list(scratch) + ([pltpu.SemaphoreType.DMA((len(plan), 2, GATHER_SEMS))] if plan else []),
        input_output_aliases={n_in + i: n_out + i for i in range(n)},
        compiler_params=pltpu.CompilerParams(vmem_limit_bytes=LIMIT, collective_id=cid, has_side_effects=bool(plan)),
        cost_estimate=pl.CostEstimate(flops=flops, bytes_accessed=flops // 1000, transcendentals=0),
    )(*ins, *extra)
    for name, new in zip(names, got[n_out:]):
        arrays[name] = new
    return got[:n_out]


def prologue_body(pack_ref, wo_ref, wd_ref, coarse_ref, fine_ref, cos_ref, sin_ref, qkv0, qkv1, gu0, gu1, wo0, wo1, wd0, wd1, theirs, merged, xs, ls, sems):
    pos = place()
    c, me = pos["c"], LINES * pos["own"] + pos["z"]
    greet(pos)
    across = [remote(pack_ref.at[1 - c, n], theirs.at[n], xs, n, pos["peer"]["d"]) for n in range(CORES)]
    for copy in across:
        copy.start()
    local = [pltpu.make_async_copy(w.at[n], ref.at[me, c], ls.at[i, n]) for i, (w, refs) in enumerate(((wo_ref, (wo0, wo1)), (wd_ref, (wd0, wd1)))) for n, ref in enumerate(refs)]
    for copy in local:
        copy.start()

    def merge(n, first, last):
        for at in range(first, last, TILE):
            cols = slice(at, at + TILE)
            mine, other = pack_ref[c, n, :, cols].astype(f32), theirs[n, :, cols].astype(f32)
            top, low = jnp.where(c == 0, mine, other), jnp.where(c == 0, other, mine)
            both = jnp.concatenate([top, low], 0)
            moved = pltpu.roll(both, both.shape[0] - (top.shape[0] - OWN), 0)
            row = lax.broadcasted_iota(jnp.int32, both.shape, 0)
            merged[n, :, cols] = jnp.where(row < OWN, both, moved)[:PAIR].astype(bf16)

    def put(ref, n, first, size, i):
        copy = pltpu.make_async_copy(merged.at[n, :, pl.ds(first, size)], ref.at[c, block(me, PAIR)], ls.at[2 + i, n])
        copy.start()
        return copy

    halves = [Gather(pos, qkv0, (i * HD, HD), sems.at[i]) for i in range(LINES)]
    later = [Gather(pos, gu0, (F // LINES * i, F // LINES), sems.at[LINES + i]) for i in range(CORES)]
    across[0].wait()
    merge(0, 0, WIDE)
    put(qkv0, 0, 0, WIDE, 0).wait()
    for part in halves:
        part.start("z")
    merge(0, WIDE, WIDE + F)
    there = put(gu0, 0, WIDE, F, 1)
    across[1].wait()
    merge(1, 0, WIDE + F)
    rest = [there, put(qkv1, 1, 0, WIDE, 0), put(gu1, 1, WIDE, F, 1)]
    there.wait()
    for part in later:
        part.start("z")
    for part in halves:
        part.wait("z")
        part.start("ab", "near")
    fine, big = fine_ref[:], coarse_ref[:]
    n = fine.shape[1]
    for i in range(T // n):
        rows = slice(i * n, i * n + n)
        ca, sa = big[0, i : i + 1], big[1, i : i + 1]
        cos_ref[rows] = ca * fine[0] - sa * fine[1]
        sin_ref[rows] = sa * fine[0] + ca * fine[1]
    for part in halves:
        part.wait("ab")
        part.start("far", "mid")
    for part in halves:
        part.wait("far")
        part.start("last")
    for copy in local + rest[1:]:
        copy.wait()
    for part in halves:
        part.wait("near", "mid", "last")
    for part in later:
        part.wait("z")


def prologue(pack, wo, wd, coarse, fine):
    rows = pack.shape[2]
    full = [shape(CORES, D, WIDE)] * 2 + [shape(CORES, D, F)] * 2 + [shape(CHIPS, 2, wo.shape[1], D)] * 2 + [shape(CHIPS, 2, wd.shape[1], D)] * 2
    table = [shape(T, HALF, dtype=f32)] * 2
    whole = lambda a: const(*a.shape)
    got = pl.pallas_call(
        prologue_body, grid=(1,), in_specs=[whole(a) for a in (pack, wo, wd, coarse, fine)],
        out_specs=[whole(a) for a in table] + [HBM] * len(full), out_shape=table + full,
        scratch_shapes=[pltpu.VMEM((CORES, rows, pack.shape[3]), bf16), pltpu.VMEM((CORES, PAIR, pack.shape[3]), bf16), pltpu.SemaphoreType.DMA((CORES, 2)),
                        pltpu.SemaphoreType.DMA((LINES, 2)), pltpu.SemaphoreType.DMA((6, 2, GATHER_SEMS))],
        compiler_params=pltpu.CompilerParams(vmem_limit_bytes=LIMIT, collective_id=0, has_side_effects=True),
    )(pack, wo, wd, coarse, fine)
    return got[0], got[1], dict(zip(("qkv0", "qkv1", "gu0", "gu1", "wo0", "wo1", "wd0", "wd1"), got[2:]))


def turn(t, cos, sin):
    x, y = t[:, :HALF].astype(f32), t[:, HALF:].astype(f32)
    return jnp.concatenate([x * cos - y * sin, y * cos + x * sin], -1).astype(bf16)


def project_body(h_ref, w_ref, cos_ref, sin_ref, q_ref, k_ref, v_ref):
    a = normed(h_ref[:])
    cos, sin = cos_ref[:], sin_ref[:]
    for n, (owner, at, ref, head) in enumerate(((0, 0, q_ref, 0), (0, TILE, q_ref, 2), (1, 0, k_ref, 0), (1, TILE, v_ref, 0))):
        r = dot(a, w_ref[owner, :, at : at + TILE]).astype(bf16)
        for i in range(CORES):
            t = r[:, i * HD : i * HD + HD]
            ref[head + i] = turn(t, cos, sin) if ref is not v_ref else t


def project(h, w, cos, sin, *ride):
    rows = lambda width: along(0, TILE, width)
    heads = (HEADS, CORES, CORES)
    return call(project_body, (T // TILE,), (h, w, cos, sin), [rows(D), const(*w.shape), rows(HALF), rows(HALF)],
                [along(1, n, TILE, HD) for n in heads], [shape(n, T, HD) for n in heads], [], T * D * T * 2, *ride)


HIDDEN = -2e30
SCALE = HD**-0.5
EXP = SCALE * 1.4426950408889634
PIECES = [(i, n) for i in range(CORES) for n in range(CORES)]


def attend_body(q_ref, k_ref, v_ref, o_ref, lse_ref, top_s, mix_s):
    iq = pl.program_id(0)
    top_s[:] = jnp.full(top_s.shape, HIDDEN / 2, f32)
    mix_s[:] = jnp.zeros(mix_s.shape, f32)
    ones = jnp.ones((8, TILE), bf16)

    def keys(j, masked):
        here = block(j, TILE)
        scores = [dot_t(k_ref[i, here, :], q_ref[2 * i + n]) for i, n in PIECES]
        weights, keeps = [], []
        for m, s in enumerate(scores):
            if masked:
                s = jnp.where(lax.broadcasted_iota(jnp.int32, s.shape, 1) >= lax.broadcasted_iota(jnp.int32, s.shape, 0), s, HIDDEN)
            old = top_s[m : m + 1, :]
            top = jnp.maximum(old, s.max(axis=0, keepdims=True))
            top_s[m : m + 1, :] = top
            weights.append(jnp.exp2((s - top) * EXP).astype(bf16))
            keeps.append(jnp.exp2((old - top) * EXP))
        for m, (i, _) in enumerate(PIECES):
            values = jnp.concatenate([v_ref[i, here, :].T, ones], axis=0)
            mix_s[m] = mix_s[m] * keeps[m] + dot(values, weights[m])

    lax.fori_loop(0, iq, lambda j, _: keys(j, False), None)
    keys(iq, True)
    for m in range(len(PIECES)):
        total = mix_s[m, HD : HD + 1, :]
        o_ref[m] = (mix_s[m, :HD, :] * (1 / total)).T.astype(bf16)
        lse_ref[m] = top_s[m : m + 1, :] * SCALE + jnp.log(total)


def attend(q, k, v, *ride):
    tile = along(1, HEADS, TILE, HD)
    return call(attend_body, (T // TILE,), (q, k, v), [tile, const(*k.shape), const(*v.shape)],
                [tile, along(2, HEADS, 1, TILE)], [shape(HEADS, T, HD), shape(HEADS, 1, T, dtype=f32)],
                [pltpu.VMEM((HEADS, TILE), f32), pltpu.VMEM((HEADS, HD + 8, TILE), f32)], 4 * 2 * T * T * HD, *ride)


def gate_up_body(o_ref, wo_ref, h_ref, wg_ref, wu_ref, h2_ref, g_ref, u_ref, p_ref, b_s):
    j, t = pl.program_id(0), pl.program_id(1)
    tm = g_ref.shape[0]

    @pl.when(j == 0)
    def _():
        rows = block(t, tm)
        acc = sum(dot(o_ref[n, rows, :], wo_ref[4 * n : 4 * n + 4].reshape(HD, D)) for n in range(LINES))
        h2 = h_ref[rows] + acc.astype(bf16)
        h2_ref[rows] = h2
        b_s[rows] = normed(h2)

    sub = 256
    for m in range(tm // sub):
        here = cut(m, sub)
        b = b_s[block(t * (tm // sub) + m, sub), :]
        g, u = dot(b, wg_ref[0]), dot(b, wu_ref[0])
        g_ref[here] = g
        u_ref[here] = u
        p_ref[here] = (g * jax.nn.sigmoid(g) * u).astype(bf16)


def gate_up(o, wo, h, gu, *ride):
    tm = 1024
    tile = pl.BlockSpec((tm, TILE), lambda j, t: (t, j))
    weight = lambda i: pl.BlockSpec((1, D, TILE), lambda j, t: (i, 0, j))
    return call(gate_up_body, (F // TILE, T // tm), (o, wo, h, gu, gu), [const(*o.shape), const(*wo.shape), const(*h.shape), weight(0), weight(1)],
                [const(T, D), tile, tile, tile], [shape(T, D), shape(T, F, dtype=f32), shape(T, F, dtype=f32), shape(T, F)],
                [pltpu.VMEM((T, D), bf16)], 2 * T * D * (D + 2 * F), *ride)


def down_body(p_ref, wd_ref, h2_ref, h3_ref):
    acc = dot(p_ref[:], wd_ref[:])
    h3_ref[:] = h2_ref[:] + acc.astype(bf16)


def down(p, wd, h2, *ride):
    rows = lambda n: along(0, TILE, n)
    return call(down_body, (T // TILE,), (p, wd.reshape(F, D), h2), [rows(F), const(F, D), rows(D)], [rows(D)], [shape(T, D)], [], 2 * T * D * F, *ride)


PLANS = (
    dict(
        project=("gu0[0:2],ab.0.1,far.1.3,last.3.e", "gu0[2:4],ab.0.2,far.2.e,last.e.e", "gu0[4:8],z.0.e", "wo0,z.0.e"),
        attend=("wo0,ab.0.1,far.1.2,last.2.e", "gu0[4:8],ab.0.2,far.2.e,last.e.e", "wd0,z.0.e"),
        gate_up=("wd0,ab.0.5,far.5.9,last.9.e", "qkv1,z.0.5,ab.5.e", "gu1[0:2],z.5.9,ab.9.e", "gu1[2:4],z.5.e"),
        down=("qkv1,far.0.2,last.2.e", "gu1[0:2],far.0.e", "gu1[2:4],ab.0.e", "gu1[4:6],z.0.e"),
    ),
    dict(
        project=("gu1[0:2],last.0.e", "gu1[2:4],far.0.e", "gu1[4:6],ab.0.e", "gu1[6:8],z.0.e", "wo1,z.0.e"),
        attend=("gu1[2:4],last.0.e", "gu1[4:6],far.0.3,last.3.e", "gu1[6:8],ab.0.3,far.3.e,last.e.e", "wo1,ab.0.3,far.3.e,last.e.e", "wd1,z.0.e"),
        gate_up=("wd1,ab.0.6,far.6.10,last.10.e",),
    ),
)


def read_plan(text):
    name, *todo = text.split(",")
    name, _, cols = name.rstrip("]").partition("[")
    if cols:
        first, end = (F // 8 * int(n) for n in cols.split(":"))
        cols = (first, end - first)
    phases = [item.split(".") for item in todo]
    return name, cols, {phase: [END if k == "e" else int(k) for k in steps] for phase, *steps in phases}


def forward(x, pack, wo, wd, coarse, fine):
    cos, sin, arrays = prologue(pack, wo, wd, coarse, fine)
    h, kept, cid = x, [], 1
    for n, texts in enumerate(PLANS):
        plan = {name: [read_plan(item) for item in text] for name, text in texts.items()}
        q, k, v = project(h, arrays[f"qkv{n}"], cos, sin, arrays, plan["project"], cid)
        o, lse = attend(q, k, v, arrays, plan["attend"], cid + 1)
        h2, g, u, p = gate_up(o, arrays[f"wo{n}"], h, arrays[f"gu{n}"], arrays, plan["gate_up"], cid + 2)
        kept.append((h, q, k, v, o, lse, h2, g, u, p))
        if n == 0:
            h, = down(p, arrays["wd0"], h2, arrays, plan["down"], cid + 3)
        cid += 4
    return cos, sin, arrays, kept


def ring_scratch(rows, width, slots, late=0):
    line = LINES * rows
    dims = ((slots, CORES, LINES * line), (slots, LINES * line), (slots, CORES, line), (slots, line), (late or slots, LINES, rows), (slots, LINES - 1, rows))
    return [pltpu.VMEM((*d, width), bf16) for d in dims] + [pltpu.SemaphoreType.DMA((slots, 2, 7))]


RING = 7


class Ring:
    def __init__(self, pos, refs):
        self.pos = pos
        self.my, self.rd, self.rb, self.ra, self.zs, self.rz, self.sems = refs
        self.rows = self.zs.shape[2]
        self.late = lambda slot: jnp.minimum(slot, self.zs.shape[0] - 1)

    def line(self, l):
        return block(l, LINES * self.rows)

    def copies(self, slot, stage, source=None):
        p, peer, sems = self.pos, self.pos["peer"], self.sems.at[slot]
        mine = self.my.at[slot, p["c"]]
        if stage == 0:
            source = self.my.at[slot] if source is None else source
            return [remote(source.at[1 - p["c"]], self.rd.at[slot], sems, 0, peer["d"])]
        if stage == 1:
            return [remote(mine.at[self.line(p[name])], self.rb.at[slot, i], sems, 1 + i, peer["b"]) for i, name in enumerate(("lb", "ld"))]
        if stage == 2:
            return [remote(mine.at[self.line(p["la"])], self.ra.at[slot], sems, 3, peer["a"])]
        return [remote(self.zs.at[self.late(slot), lax.rem(p["z"] + k, LINES)], self.rz.at[slot, k - 1], sems, 3 + k, peer[k]) for k in range(1, LINES)]

    def send(self, slot, stage=0, source=None):
        for copy in self.copies(slot, stage, source):
            copy.start()

    def add(self, slot, l, theirs):
        n, size = LINES * self.rows, 32
        c = self.pos["c"]

        def some(i, _):
            here, there = pl.ds(pl.multiple_of(n * l + i * size, size), size), pl.ds(pl.multiple_of(i * size, size), size)
            self.my[slot, c, here, :] = (self.my[slot, c, here, :].astype(f32) + theirs[there, :].astype(f32)).astype(bf16)

        lax.fori_loop(0, n // size, some, None)

    def stage(self, slot, n):
        p = self.pos
        for copy in self.copies(slot, n - 1):
            copy.wait()
        if n == 1:
            for l in range(LINES):
                self.add(slot, l, self.rd.at[slot, self.line(l)])
        elif n == 2:
            self.add(slot, p["own"], self.rb.at[slot, 0])
            self.add(slot, p["la"], self.rb.at[slot, 1])
        elif n == 3:
            mine = self.my[slot, p["c"], self.line(p["own"]), :].astype(f32)
            self.zs[self.late(slot)] = (mine + self.ra[slot].astype(f32)).reshape(LINES, self.rows, -1).astype(bf16)
        else:
            return (self.zs[self.late(slot), p["z"]].astype(f32) + sum(self.rz[slot, k].astype(f32) for k in range(LINES - 1))).astype(bf16)
        self.send(slot, n)


def drain(units):
    while units:
        for ring, slot, n, end in units:
            ring.stage(slot, n) if n < 4 else end()
        units = [(ring, slot, n + 1, end) for ring, slot, n, end in units if n < 4]


def finish(copies):
    for copy in copies:
        copy.wait()


def ffn_back_body(h2_ref, dy_ref, p_ref, g_ref, u_ref, wg_ref, wu_ref, wd_ref, o_ref, wo_ref, fin, late_out, wd_out, dh_ref, do_ref, dwo_ref,
                  b_s, db_s, dg_s, du_s, ls, *rest):
    j, t = pl.program_id(0), pl.program_id(1)
    tm, nj, nt = g_ref.shape[0], pl.num_programs(0) - 1, pl.num_programs(1) - 1
    pos = place()
    gu, wd = Ring(pos, rest[:RING]), Ring(pos, rest[RING:])
    slot, old = lax.rem(j, 2), lax.rem(j + 1, 2)
    third = lambda n: lax.rem(n, 3)
    n_last = F // TILE - 1
    final = third(n_last)
    newest, oldest = third(j + 2), third(j + 1)
    at = lambda k, *also: functools.partial(pl.when, functools.reduce(lambda a, b: a & b, also, t == k))()
    at(0, j == 0)(lambda: greet(pos))
    sub = 256
    both, ours, late = j >= 2, (j >= 1) & (j < nj), j == nj - 1

    def gu_end():
        fin[:, block(j - 2, TILE)] = gu.stage(slot, 4)

    def wd_end(j):
        wd_out[:, block(j, HALF)] = wd.stage(third(j), 4)

    at(0, both)(lambda: wd.stage(oldest, 3))
    at(0, j == nj)(lambda: wd.stage(final, 3))
    at(0, ours)(lambda: wd.stage(newest, 1))
    at(1, both)(lambda: gu.stage(slot, 3))
    at(1, ours)(lambda: gu.stage(old, 1))
    at(1, late)(lambda: wd.stage(final, 1))

    @at(4, ours)
    def _():
        gu.stage(old, 2)
        wd.stage(newest, 2)


    at(4, both)(gu_end)
    at(4, late)(lambda: wd.stage(final, 2))
    at(4, both)(lambda: wd_end(j - 2))

    @pl.when((t < nt) & (j < nj))
    def _():
        rows = block(t, tm)

        @pl.when(j == 0)
        def _():
            b_s[rows] = normed(h2_ref[rows])
            db_s[rows] = jnp.zeros((tm, D), f32)

        for m in range(tm // sub):
            here, rows = cut(m, sub), block(t * (tm // sub) + m, sub)
            dp = dot_t(dy_ref[rows], wd_ref[:]).astype(bf16).astype(f32)
            g, u = g_ref[here], u_ref[here]
            s = jax.nn.sigmoid(g)
            gs = g * s
            du = (dp * gs).astype(bf16)
            dg = (dp * u * (s + gs * (1 - s))).astype(bf16)
            dg_s[rows] = dg
            du_s[rows] = du
            db_s[rows] += dot_t(dg, wg_ref[0]) + dot_t(du, wu_ref[0])

        @pl.when(late)
        def _():
            for m in range(tm // sub):
                rows = block(t * (tm // sub) + m, sub)
                dh_ref[rows] = norm_back(h2_ref[rows].astype(f32), db_s[rows], dy_ref[rows])

    rows = wd.rows
    for n in range(LINES):

        k = max(2 * n - 1, 0)

        @pl.when((t > 0) & (j == k))
        def _():
            r = t_dot(p_ref[:], dy_ref[:, HALF * k : sub * n + HALF]).astype(bf16)
            for q in range(D // rows):
                at = pl.multiple_of(LINES * rows * (t - 1) + rows * (q // CORES), rows)
                for e in range(r.shape[1] // HALF):
                    wd.my[third(k + e), q % CORES, pl.ds(at, rows), :] = r[cut(q, rows), cut(e, HALF)]

    at(4, j < nj, ~late)(lambda: wd.send(third(j)))
    at(4, j == nj - 2)(lambda: wd.send(final))

    @at(4, j < nj)
    def _():
        for i, ref in enumerate((dg_s, du_s)):
            for n in range(TILE // sub):
                cols = cut(n, sub)
                gu.my[slot, i, :, cols] = t_dot(b_s[:], ref[:, cols]).astype(bf16)
        pl.when(j < nj - 1)(lambda: gu.send(slot))

    save = pltpu.make_async_copy(gu.my.at[n_last % 2], late_out, ls)
    at(4, late)(lambda: save.start())

    @pl.when((j == nj) & (t < nt))
    def _():
        do_ref[0] = dot_t(dh_ref[:], wo_ref[:].reshape(HD, D)).astype(bf16)
        r = t_dot(o_ref[0], dh_ref[:]).astype(bf16).reshape(*wo_ref.shape)
        for i in range(CORES):
            dwo_ref[i] = r[:, i].reshape(HALF, D)

    @at(4, j == nj)
    def _():
        wd_end(n_last)
        save.wait()


def ffn_back(h2, dy, p, g, u, gu, wd, o, wo, cid):
    tm = 512
    nj, nt = F // TILE, T // tm
    tj = lambda j: jnp.minimum(j, nj - 1)
    tt = lambda j, t: jnp.where(j < nj, jnp.minimum(t, nt - 1), nt - 1)
    head = lambda j, t: jnp.where(j < nj, 0, jnp.minimum(t, nt - 1))
    weight = lambda i: pl.BlockSpec((1, D, TILE), lambda j, t: (i, 0, tj(j)))
    tile = pl.BlockSpec((tm, TILE), lambda j, t: (tt(j, t), tj(j)))
    one = pl.BlockSpec((1, T, HD), lambda j, t: (head(j, t), 0, 0))
    rows, done = F // CHIPS // CORES, F - TILE
    return pl.pallas_call(
        ffn_back_body, grid=(nj + 1, nt + 1),
        in_specs=[const(T, D), const(T, D), pl.BlockSpec((T, D), lambda j, t: (0, jnp.where((j == 0) | (lax.rem(j, 2) > 0), jnp.maximum(t - 1, 0), nt - 1))), tile, tile,
                  weight(0), weight(1), pl.BlockSpec((TILE, D), lambda j, t: (tj(j), 0)), one,
                  pl.BlockSpec((4, *wo.shape[1:]), lambda j, t: (head(j, t), 0, 0, 0))],
        out_specs=[const(PAIR, done), HBM, const(rows, D), const(T, D), one, pl.BlockSpec((CORES, HALF, D), lambda j, t: (0, head(j, t), 0))],
        out_shape=[shape(PAIR, done), shape(CORES, D, TILE), shape(rows, D), shape(T, D), shape(HEADS, T, HD), shape(CORES, TILE, D)],
        scratch_shapes=[pltpu.VMEM((T, D), bf16), pltpu.VMEM((T, D), f32), pltpu.VMEM((T, TILE), bf16), pltpu.VMEM((T, TILE), bf16)]
        + [pltpu.SemaphoreType.DMA(())] + ring_scratch(PAIR, TILE, 2, 1) + ring_scratch(rows, HALF, 3, 2),
        compiler_params=pltpu.CompilerParams(vmem_limit_bytes=LIMIT, collective_id=cid, has_side_effects=True),
        cost_estimate=pl.CostEstimate(flops=12 * T * D * F, bytes_accessed=F * T * 12, transcendentals=0),
    )(h2, dy, p, g, u, gu, gu, wd.reshape(F, D), o, wo)


DUE = ((4, 6), (6, 8), (7, 8), (8,))


def attend_back_body(q_ref, k_ref, v_ref, do_ref, o_ref, lse_ref, wo_in, *refs, units):
    given, refs = refs[:units], refs[units:]
    dq_ref, dk_ref, dv_ref, wo_out, fin, dq_s, dk_s, dv_s, delta_s, loads, *rest = refs
    iq = pl.program_id(0)
    pos = place()
    wide, wo = Ring(pos, rest[:RING]), Ring(pos, rest[RING:])
    todo = [(wide, 0, given[0]), (wo, 0, wo_in)] + [(wide, 1 + i, ref.at[i]) for ref in given[1:] for i in range(CORES)]
    mine = [pltpu.make_async_copy(ref.at[pos["c"]], ring.my.at[slot, pos["c"]], loads.at[i]) for i, (ring, slot, ref) in enumerate(todo)]

    def end(ring, slot):
        if ring is wo:
            wo_out[:] = ring.stage(slot, 4)
        else:
            fin[:, TILE * slot : TILE * slot + TILE] = ring.stage(slot, 4)

    def event(e):
        @pl.when(e == 1)
        def _():
            for copy, (ring, slot, _) in zip(mine, todo):
                copy.wait()
                ring.stage(slot, 1)

        for (ring, slot, _), steps in zip(todo, DUE):
            for n, k in enumerate(steps):
                pl.when(e == k)(functools.partial(ring.stage, slot, n + 2))

    @pl.when(iq == 0)
    def _():
        for copy in mine:
            copy.start()
        greet(pos)
        for ring, slot, ref in todo:
            ring.send(slot, 0, ref)
        dk_s[:] = jnp.zeros_like(dk_s)
        dv_s[:] = jnp.zeros_like(dv_s)

    dq_s[:] = jnp.zeros_like(dq_s)
    for m in range(len(PIECES)):
        x = do_ref[m].astype(f32) * o_ref[m].astype(f32)
        delta_s[m] = (x[:, :HALF] + x[:, HALF:]).T.sum(axis=0, keepdims=True)

    def keys(j, masked):
        here = block(j, TILE)
        scores = [dot_t(k_ref[i, here, :], q_ref[2 * i + n]) for i, n in PIECES]
        dps = [dot_t(v_ref[i, here, :], do_ref[2 * i + n]) for i, n in PIECES]
        for m, (i, n) in enumerate(PIECES):
            p = jnp.exp2(scores[m] * EXP - lse_ref[m] * (EXP / SCALE))
            if masked:
                p = jnp.where(lax.broadcasted_iota(jnp.int32, p.shape, 1) >= lax.broadcasted_iota(jnp.int32, p.shape, 0), p, 0.0)
            ds = (p * (dps[m] - delta_s[m])).astype(bf16)
            dv_s[i, here, :] += dot(p.astype(bf16), do_ref[m])
            dk_s[i, here, :] += dot(ds, q_ref[m])
            dq_s[m] += dot(k_ref[i, here, :].T, ds)

    @functools.partial(lax.fori_loop, 0, iq, init_val=None)
    def _(j, _):
        event(lax.div(iq * (iq + 1), 2) + j)
        keys(j, False)

    keys(iq, True)
    for m in range(len(PIECES)):
        dq_ref[m] = (dq_s[m] * SCALE).T.astype(bf16)

    @pl.when(iq == pl.num_programs(0) - 1)
    def _():
        dk_ref[:] = (dk_s[:] * SCALE).astype(bf16)
        dv_ref[:] = dv_s[:].astype(bf16)
        drain([(ring, slot, 2 + len(steps), functools.partial(end, ring, slot)) for (ring, slot, _), steps in zip(todo, DUE)])


def attend_back(q, k, v, do, o, lse, dwo, units, cid):
    tile = along(1, HEADS, TILE, HD)
    keys, rows, n = const(*k.shape), D // OWN, len(units)
    n_wide = CORES * n - 1
    return pl.pallas_call(
        functools.partial(attend_back_body, units=n), grid=(T // TILE,),
        in_specs=[tile, keys, keys, tile, tile, along(2, HEADS, 1, TILE)] + [HBM] * (1 + n),
        out_specs=[tile, keys, keys, const(rows, D), const(PAIR, n_wide * TILE)],
        out_shape=[shape(*a.shape) for a in (q, k, v)] + [shape(rows, D), shape(PAIR, n_wide * TILE)],
        scratch_shapes=[pltpu.VMEM((HEADS, HD, TILE), f32), pltpu.VMEM(k.shape, f32), pltpu.VMEM(k.shape, f32), pltpu.VMEM((HEADS, 1, TILE), f32)]
        + [pltpu.SemaphoreType.DMA((1 + n_wide,))] + ring_scratch(PAIR, TILE, n_wide) + ring_scratch(rows, D, 1),
        compiler_params=pltpu.CompilerParams(vmem_limit_bytes=LIMIT, collective_id=cid, has_side_effects=True),
        cost_estimate=pl.CostEstimate(flops=20 * T * T * HD, bytes_accessed=T * D * 12, transcendentals=0),
    )(q, k, v, do, o, lse, dwo, *units)


def turn_back(ref, g_s, first, *angles):
    sub = 512
    for i in range(ref.shape[0]):
        at = first + i * HD
        for m in range(0, T, sub):
            rows = slice(m, m + sub)
            t = ref[i, rows, :]
            g_s[rows, at : at + HD] = turn(t, angles[0][rows], -angles[1][rows]) if angles else t


def qkv_back_body(dq_ref, dk_ref, dv_ref, cos_ref, sin_ref, h_ref, w_ref, dh2_ref, dw_ref, dh_ref, a_s, g_s, da_s):
    s = pl.program_id(0)
    sub = 512
    pieces = [slice(m, m + sub) for m in range(0, T, sub)]

    @pl.when(s == 0)
    def _():
        for m in pieces:
            a_s[m] = normed(h_ref[m])
            da_s[m] = jnp.zeros((sub, D), f32)

    for k, ref in enumerate((dq_ref, dk_ref, dq_ref, dv_ref)):
        angles = () if ref is dv_ref else (cos_ref, sin_ref)
        pl.when(s == k)(functools.partial(turn_back, ref, g_s, 0, *angles))
    dw_ref[0, 0] = t_dot(a_s[:], g_s[:]).astype(bf16)
    for m in pieces:
        da_s[m] += dot_t(g_s[m], w_ref[0])

    @pl.when(s == 3)
    def _():
        for m in pieces:
            dh_ref[m] = norm_back(h_ref[m].astype(f32), da_s[m], dh2_ref[m])


def qkv_back(dq, dk, dv, cos, sin, h, w, dh2):
    keys = const(*dk.shape)
    return call(qkv_back_body, (HEADS,), (dq, dk, dv, cos, sin, h, w, dh2),
                [pl.BlockSpec((CORES, T, HD), lambda s: (lax.div(s, 2), 0, 0)), keys, keys, const(T, HALF), const(T, HALF), const(T, D),
                 pl.BlockSpec((1, D, TILE), lambda s: (lax.rem(s, 2), 0, lax.div(s, 2))), const(T, D)],
                [pl.BlockSpec((1, 1, D, TILE), lambda s: (lax.div(s, 2), lax.rem(s, 2), 0, 0)), const(T, D)], [shape(CORES, 2, D, TILE), shape(T, D)],
                [pltpu.VMEM((T, D), bf16), pltpu.VMEM((T, TILE), bf16), pltpu.VMEM((T, D), f32)], 4 * T * D * 4 * TILE)


def qkv_last_body(dq_ref, dk_ref, dv_ref, cos_ref, sin_ref, h_ref, fin, a_s, g_s, *rest):
    pos = place()
    ring = Ring(pos, rest)
    s = pl.program_id(0)

    @pl.when(s == 0)
    def _():
        greet(pos)
        a_s[:] = normed(h_ref[:])

    turn_back(dq_ref, g_s, 0, cos_ref, sin_ref)
    pl.when(s < 2)(lambda: turn_back(dk_ref, g_s, HD, cos_ref, sin_ref))
    pl.when(s >= 2)(lambda: turn_back(dv_ref, g_s, HD))
    for i in range(CORES):
        ring.my[s, i] = t_dot(a_s[:], g_s[:, HD * i : HD * i + HD]).astype(bf16)
    ring.send(s)

    def end(slot):
        fin[:, HD * slot : HD * slot + HD] = ring.stage(slot, 4)

    for k in range(1, 4):
        for n in range(1, k + 1):
            pl.when(s == k)(functools.partial(ring.stage, k - n, n))

    @pl.when(s == 3)
    def _():
        drain([(ring, slot, 4 - slot, functools.partial(end, slot)) for slot in range(LINES)])


def qkv_last(dq, dk, dv, cos, sin, h, cid):
    head = lambda n, of: pl.BlockSpec((1, T, HD), lambda s: (jnp.clip(s - n, 0, of - 1), 0, 0))
    return pl.pallas_call(
        qkv_last_body, grid=(HEADS,), in_specs=[head(0, 4), head(0, 2), head(2, 2), const(T, HALF), const(T, HALF), const(T, D)], out_specs=const(PAIR, WIDE),
        out_shape=shape(PAIR, WIDE),
        scratch_shapes=[pltpu.VMEM((T, D), bf16), pltpu.VMEM((T, TILE), bf16)] + ring_scratch(PAIR, HD, 4),
        compiler_params=pltpu.CompilerParams(vmem_limit_bytes=LIMIT, collective_id=cid, has_side_effects=True),
        cost_estimate=pl.CostEstimate(flops=2 * T * D * 4 * TILE, bytes_accessed=T * D * 10, transcendentals=0),
    )(dq, dk, dv, cos, sin, h)


def sources(gu, late, qkv, first):
    wide = F - TILE
    pair = lambda owner: [(gu, owner, 0, 0, wide), (late, owner, 0, wide, TILE)]
    return [[(qkv, 0, first, 0, WIDE)], [(qkv, 1, first, 0, TILE)], [(qkv, 1, first + TILE, 0, TILE)], pair(0), pair(1)]


def own_rows(c, both, owner, cols):
    mine, theirs = (ref[:, cols].astype(f32) for ref in both)
    x = jnp.where(c == owner, mine, theirs)
    return jnp.where(c == 0, x, pltpu.roll(x, OWN, 0))[:OWN]


def lay_out(c, pairs, outs):
    gu0, late0, last0, gu1, late1 = pairs
    for n, from_layer in enumerate((sources(gu0, late0, last0, 0), sources(gu1, late1, late0, TILE))):
        for out, parts in zip(outs, from_layer):
            for ref, owner, at, to, width in parts:
                for k in range(0, width, TILE):
                    out[:, n, to + k : to + k + TILE] = own_rows(c, ref, owner, slice(at + k, at + k + TILE))


def squares_body(*refs, n_sums, n_halved):
    sums, out_ref, grads = refs[:n_sums], refs[n_sums], refs[n_sums + 1 : -4 - n_halved]
    *others, mine, parts, swap, sems = refs[-4 - n_halved :]
    pos = place()
    greet(pos)
    halved = sums[:n_halved]
    across = [remote(ref, other, swap, i, pos["peer"]["d"]) for i, (ref, other) in enumerate(zip(halved, others))]
    for copy in across:
        copy.start()
    total = jnp.zeros((1, HALF), f32)
    for ref in sums:
        for at in range(0, ref.shape[1], HALF):
            x = ref[:, at : at + HALF].astype(f32)
            total += (x * x).sum(axis=0, keepdims=True)
    mine[:] = jnp.broadcast_to(total, mine.shape)
    n = 0
    for names in ("d", "a", "b", range(1, LINES)):
        copies = [remote(mine, parts.at[n + i], sems, n + i, pos["peer"][name]) for i, name in enumerate(names)]
        for copy in copies:
            copy.start()
        if n == 1:
            finish(across)
            lay_out(pos["c"], list(zip(halved, others)), grads)
        finish(copies)
        mine[:] += sum(parts[n + i] for i in range(len(names)))
        n += len(names)
    out_ref[:] = mine[:]


def squares(halved, whole, cid):
    part, peers, sums = (8, HALF), LINES + 2, (*halved, *whole)
    outs = [shape(*part, dtype=f32)] + [shape(OWN, 2, n, dtype=f32) for n in (WIDE, TILE, TILE, F, F)]
    return pl.pallas_call(
        functools.partial(squares_body, n_sums=len(sums), n_halved=len(halved)), grid=(1,), in_specs=[const(*a.shape) for a in sums],
        out_specs=[const(*a.shape) for a in outs], out_shape=outs,
        scratch_shapes=[pltpu.VMEM(a.shape, bf16) for a in halved]
        + [pltpu.VMEM(part, f32), pltpu.VMEM((peers, *part), f32), pltpu.SemaphoreType.DMA((CORES, len(halved))), pltpu.SemaphoreType.DMA((CORES, peers))],
        compiler_params=pltpu.CompilerParams(vmem_limit_bytes=LIMIT, collective_id=cid, has_side_effects=True),
    )(*sums)


def adamw(w, m, v, g):
    m = 0.9 * m + 0.1 * g
    v = 0.95 * v + 0.05 * g * g
    step = m * lax.rsqrt(v + 1e-8) + 0.1 * w
    return (w - 0.02 * step).astype(bf16), m, v


def update(halved, whole, weights, m, v, cid):
    total, *grads = squares(halved, whole, cid)
    count = 2 * CHIPS * sum(w.size for w in weights)
    factor = jnp.minimum(1.0, 0.5 * lax.rsqrt(total[0].sum() / count + 1e-30))
    q, k, vv, gate, up = (g.transpose(1, 0, 2) for g in grads)
    o0, d0, o1, d1 = whole
    both = lambda *layers: jnp.stack(layers).astype(f32)
    grads = q, k, vv, both(o0, o1), gate, up, both(d0, d1)
    new = [adamw(w.astype(f32), m, v, g * factor) for w, m, v, g in zip(weights, m, v, grads, strict=True)]
    return tuple(one[which] for which in range(3) for one in new)


def tables():
    freq, fine = THETA ** (-jnp.arange(HALF, dtype=f32) / HALF), 64
    angles = [jnp.arange(n, dtype=f32)[:, None] * step * freq for n, step in ((T // fine, fine), (fine, 1))]
    return [jnp.stack([jnp.cos(a), jnp.sin(a)]) for a in angles]


def solution(mesh):
    def step(x, dy, *arrays):
        wq, wk, wv, wo, wg, wu, wd = arrays[:7]
        pack = jnp.stack([jnp.pad(jnp.concatenate(parts, -1), ((0, 0), (0, 4), (0, 0))) for parts in ((wq, wg), (wk, wv, wu))])
        cos, sin, full, kept = forward(x[0], pack, wo, wd, *tables())
        by_h, late, halved, whole = dy[0], [], [], []
        for n in (1, 0):
            h, q, k, vv, o, lse, h2, g, u, p = kept[n]
            s_gu, last, s_d, dh2, do, dwo = ffn_back(h2, by_h, p, g, u, full[f"gu{n}"], full[f"wd{n}"], o, full[f"wo{n}"], 8)
            dq, dk, dv, s_o, s_late = attend_back(q, k, vv, do, o, lse, dwo, [last, *late], 9 + n)
            if n:
                dqkv, by_h = qkv_back(dq, dk, dv, cos, sin, h, full[f"qkv{n}"], dh2)
                late = [dqkv]
            last = [] if n else [qkv_last(dq, dk, dv, cos, sin, h, 11)]
            halved, whole = [s_gu, s_late, *last, *halved], [s_o, s_d, *whole]
        return update(halved, whole, *(arrays[i : i + 7] for i in (0, 7, 14)), 12)

    states, cut = P(("rep", "dp")), P(None, "dp")
    return jax.shard_map(step, mesh=mesh, in_specs=(states, states) + (cut,) * 21, out_specs=(P("rep", "dp"),) * 21, check_vma=False)
```
